512 devices in a mesh: fy: 16 (over y, core), fx: 16 (over z, x_hi), blk: 2 (over x_lo).
Axes of the slice: x: 4 (x_hi: 2, x_lo: 2; x = x_hi * 2 + x_lo), y: 8, z: 8, core: 2. Of those that a mesh axis runs over, the one named last changes fastest.
Arguments:
- sky_image: bfloat16 [8, 2048, 2048], P('blk', 'fy', 'fx'), may hold values from -33 to 33
- vis_data: bfloat16 [16, 16, 8, 2, 512], P('fy', 'fx', 'blk'), may hold values from -6 to 6
- interp_weights: bfloat16 [16, 16, 8, 4, 2, 128, 128], P('fy', 'fx'), may hold values from -0.125 to 0.125
- tile_rows: int32 [16, 16, 8, 4, 2], P('fy', 'fx'), may hold values from 0 to 127
- facet_list: int32 [16, 16, 8], P('fy', 'fx'), may hold values from 0 to 15, as said below
- vis_count: int32 [16, 16], P('fy', 'fx'), may hold values from 128 to 512
- wavelet_threshold: float32 [4, 8], P(None, 'blk'), may hold values from 0.05 to 0.5
- spectral_weight: float32 [], replicated, may hold values from 0.1 to 1
Outputs:
- restored: float32 [8, 2048, 2048], P('blk', 'fy', 'fx')
The draws below stay inside these ranges and needn't reach their ends.
Inputs may be any that keep to these rules, and one draw needn't show every extreme that they name: `facet_list`: the 8 facet numbers of one block are distinct.
All inputs are finite; a program needn't handle non-finite values.
Results may differ from the reference program's by a relative error of at most 0.0035.
Values may be sent and summed in bfloat16 or wider, within the bound.
A program may use at most 64 MiB of HBM per device.

```python
import math
import jax
import jax.numpy as jnp
from jax import lax

FACET = 128
CHANNELS = 8
TILE = 128
VT = 4
NNZ = 2
LEVELS = 4
NFY = 16
NFX = 16
FPB = 8
NY = 2048
NX = 2048
VIS = 512


def draw_sky_image(key, part):
    key_rows = jax.random.fold_in(key, 11)
    key_cols = jax.random.fold_in(key, 12)
    key_sky = jax.random.fold_in(key, 13)
    key_gain = jax.random.fold_in(key, 14)
    key_noise = jax.random.fold_in(key, 15)
    row_scale = jnp.exp(jax.random.uniform(key_rows, (NY, 1), jnp.float32) * math.log(3.2))
    col_scale = jnp.exp(jax.random.uniform(key_cols, (1, NX), jnp.float32) * math.log(3.2))
    sky_field = jnp.clip(jax.random.normal(key_sky, (NY, NX), jnp.float32), -4.0, 4.0)
    channel_gain = jax.random.uniform(key_gain, (CHANNELS, 1, 1), jnp.float32, 0.5, 1.5)
    channel_noise = 0.5 * jnp.clip(jax.random.normal(key_noise, (CHANNELS, NY, NX), jnp.float32), -4.0, 4.0)
    values = 0.5 * sky_field[None] * row_scale[None] * col_scale[None] * channel_gain + channel_noise
    return values.astype(jnp.bfloat16)


def draw_facet_list(key, part):
    keys_all = jax.random.split(jax.random.fold_in(key, 21), NFY * NFX)
    orders = jax.vmap(lambda block_key: jax.random.permutation(block_key, NFX))(keys_all)
    return orders[:, :FPB].reshape(NFY, NFX, FPB).astype(jnp.int32)


def touch_ends(array, own_key, smallest, largest):
    shape = array.shape
    index_at = [jax.random.randint(jax.random.fold_in(own_key, axis), (), 0, shape[axis]) for axis in range(len(shape))]
    array = array.at[tuple(index_at)].set(smallest)
    longest = shape.index(max(shape))
    index_at[longest] = (index_at[longest] + 1) % shape[longest]
    return array.at[tuple(index_at)].set(largest)


def block_levels(own_key, shape, cuts, least, top_value):
    loudness, own = 1.0, jax.random.fold_in(own_key, 6)
    for dim, blocks in cuts:
        draws = jnp.exp(jax.random.uniform(jax.random.fold_in(own, dim), (blocks,), jnp.float32, least / len(cuts), top_value / len(cuts)))
        loudness = loudness * jnp.repeat(draws, shape[dim] // blocks).reshape([-1 if axis == dim else 1 for axis in range(len(shape))])
    return loudness


def bell_draw(stream_key, extent, scale, bound, cuts=(), kind=jnp.bfloat16):
    factor_of = block_levels(stream_key, extent, cuts, -0.22, 0.18) if cuts else 1.0
    values = jax.random.normal(stream_key, extent, jnp.float32) * scale * factor_of
    return jnp.minimum(jnp.maximum(values, -bound), bound).astype(kind)


def setup_inputs(seed: int = 0) -> dict:
    streams_of = jax.random.split(jax.random.key(seed), 9)
    sky_image = draw_sky_image(jax.random.fold_in(streams_of[8], 71), 0)
    vis_data = bell_draw(streams_of[1], (NFY, NFX, CHANNELS, 2, VIS), 1.0, 6.0, ((0, 16), (1, 16), (2, 2)))
    interp_weights = bell_draw(streams_of[2], (NFY, NFX, FPB, VT, NNZ, TILE, FACET), (FPB * NNZ * FACET) ** -0.5, 0.125, ((0, 16), (1, 16)))
    tile_rows = touch_ends(jax.random.randint(streams_of[3], (NFY, NFX, FPB, VT, NNZ), 0, FACET), jax.random.fold_in(streams_of[3], 1), 0, FACET - 1).astype(jnp.int32)
    facet_list = draw_facet_list(jax.random.fold_in(streams_of[8], 71), 0)
    vis_count = touch_ends(jax.random.randint(streams_of[5], (NFY, NFX), VIS // 4, VIS + 1), jax.random.fold_in(streams_of[5], 1), VIS // 4, VIS).astype(jnp.int32)
    wavelet_threshold = jnp.clip(jnp.exp(math.log(0.5) - 2.3025851 * jax.random.uniform(streams_of[6], (LEVELS, CHANNELS), jnp.float32) ** block_levels(streams_of[6], (LEVELS, CHANNELS), ((1, 2),), -0.2, 0.2)), 0.05, 0.5)
    spectral_weight = jnp.clip(jnp.exp(jax.random.uniform(streams_of[7], (), jnp.float32, math.log(0.1), math.log(1.0))), 0.1, 1.0)
    return dict(sky_image=sky_image, vis_data=vis_data, interp_weights=interp_weights, tile_rows=tile_rows, facet_list=facet_list, vis_count=vis_count, wavelet_threshold=wavelet_threshold, spectral_weight=spectral_weight)


top_precision = lax.Precision.HIGHEST
descent_step = 2.0

def as_rounded(values):
    return lax.optimization_barrier(values.astype(jnp.bfloat16)).astype(jnp.float32)

def dft_tables(length):
    positions = jnp.arange(length, dtype=jnp.int32)
    phases = positions[:, None] * positions[None, :] % length
    angles = phases.astype(jnp.float32) * (2.0 * math.pi / length)
    scaling = 1.0 / math.sqrt(length)
    cosine = jnp.cos(angles) * scaling
    sinus_table = jnp.sin(angles) * scaling
    left_table = jnp.concatenate([cosine, -sinus_table], axis=0)
    right_table = jnp.stack([jnp.concatenate([cosine, -sinus_table], axis=1), jnp.concatenate([sinus_table, cosine], axis=1)])
    return (left_table, right_table)

def forward_transform(facets, left_table, right_table):
    halfway = jnp.einsum('wy,fcyx->fcwx', as_rounded(left_table), facets.astype(jnp.float32), precision=top_precision)
    halfway = as_rounded(halfway)
    facet_count, channel_count, doubled, facet_width = halfway.shape
    halfway = halfway.reshape(facet_count, channel_count, 2, doubled // 2, facet_width)
    spectra = jnp.einsum('fcpux,pxw->fcuw', halfway, as_rounded(right_table), precision=top_precision)
    return spectra.astype(jnp.bfloat16)

def adjoint_transform(spectrum_grad, left_table, right_table):
    halfway = jnp.einsum('fcuw,pxw->fcpux', spectrum_grad, right_table, precision=top_precision)
    facet_count, channel_count, parts_two, facet_width, other_width = halfway.shape
    halfway = halfway.reshape(facet_count, channel_count, 2 * facet_width, other_width)
    return jnp.einsum('wy,fcwx->fcyx', left_table, halfway, precision=top_precision)

def pick_rows(spectrum_one, row_ids):
    return jnp.take(spectrum_one, row_ids, axis=1)

def block_gradient(spectra, block_vis, block_weights, block_tiles, block_list, block_count):
    chosen = jnp.take(spectra, block_list, axis=0)
    picked = jax.vmap(pick_rows)(chosen, block_tiles)
    facet_count, channel_count, tile_count, slot_count, doubled = picked.shape
    picked = picked.reshape(facet_count, channel_count, tile_count, slot_count, 2, doubled // 2)
    weights_wide = block_weights.astype(jnp.float32)
    predicted = jnp.einsum('fanjv,fcanpv->cpaj', weights_wide, picked.astype(jnp.float32), precision=top_precision)
    predicted = predicted.reshape(channel_count, 2, -1)
    live_mask = jnp.arange(predicted.shape[2], dtype=jnp.int32) < block_count
    residual = jnp.where(live_mask, predicted - block_vis.astype(jnp.float32), 0.0)
    residual = as_rounded(residual).reshape(channel_count, 2, tile_count, -1)
    contrib = jnp.einsum('fanjv,cpaj->fancpv', weights_wide, residual, precision=top_precision)
    contrib = contrib.reshape(facet_count, tile_count, slot_count, channel_count, doubled)
    onehot = (block_tiles[..., None] == jnp.arange(doubled // 2, dtype=jnp.int32)).astype(jnp.float32)
    return jnp.einsum('fanu,fancw->fcuw', onehot, contrib, precision=top_precision)

def row_gradient(items):
    row_images, row_vis, row_weights, row_tiles, row_lists, row_counts = items
    left_table, right_table = dft_tables(FACET)
    spectra = forward_transform(row_images, left_table, right_table)
    block_grads = jax.vmap(block_gradient, in_axes=(None, 0, 0, 0, 0, 0))(spectra, row_vis, row_weights, row_tiles, row_lists, row_counts)
    flat_grads = block_grads.reshape((NFX * FPB,) + block_grads.shape[2:])
    row_total = jnp.zeros((NFX,) + block_grads.shape[2:], jnp.float32).at[row_lists.reshape(-1)].add(flat_grads)
    return adjoint_transform(row_total, left_table, right_table)

def smooth_axis(values, stride, axis_id):
    widths = [(0, 0), (0, 0), (0, 0)]
    widths[axis_id] = (stride, stride)
    padded = jnp.pad(values, widths)
    length = values.shape[axis_id]
    below_rows = lax.slice_in_dim(padded, 0, length, axis=axis_id)
    above_rows = lax.slice_in_dim(padded, 2 * stride, 2 * stride + length, axis=axis_id)
    return (below_rows + 2.0 * values + above_rows) * 0.25

def smooth_both(values, stride):
    return smooth_axis(smooth_axis(values, stride, 1), stride, 2)

def shrink_matrix(gram_matrix, offset):
    dimension = gram_matrix.shape[0]
    shifted = gram_matrix + offset * jnp.eye(dimension, dtype=jnp.float32)
    positions = jnp.arange(dimension, dtype=jnp.int32)
    columns = []
    for column_id in range(dimension):
        if column_id > 0:
            earlier = jnp.stack(columns, axis=1)
            correction = lax.optimization_barrier(jnp.sum(earlier * earlier[column_id][None, :], axis=1))
        else:
            correction = jnp.zeros((dimension,), jnp.float32)
        pivot = jnp.sqrt(shifted[column_id, column_id] - correction[column_id])
        column = (shifted[:, column_id] - correction) / pivot
        columns.append(jnp.where(positions >= column_id, column, 0.0))
    factor = jnp.stack(columns, axis=1)
    forward_rows = []
    for row_id in range(dimension):
        accum = gram_matrix[row_id]
        if row_id > 0:
            accum = accum - lax.optimization_barrier(jnp.sum(factor[row_id, :row_id][:, None] * jnp.stack(forward_rows, axis=0), axis=0))
        forward_rows.append(accum / factor[row_id, row_id])
    backward_rows = [None] * dimension
    for row_id in range(dimension - 1, -1, -1):
        accum = forward_rows[row_id]
        if row_id < dimension - 1:
            later = jnp.stack(backward_rows[row_id + 1:], axis=0)
            accum = accum - lax.optimization_barrier(jnp.sum(factor[row_id + 1:, row_id][:, None] * later, axis=0))
        backward_rows[row_id] = accum / factor[row_id, row_id]
    return jnp.stack(backward_rows, axis=0)

def reference(sky_image, vis_data, interp_weights, tile_rows, facet_list, vis_count, wavelet_threshold, spectral_weight):
    facets_all = sky_image.reshape(CHANNELS, NFY, FACET, NFX, FACET).transpose(1, 3, 0, 2, 4)
    gradient = lax.map(row_gradient, (facets_all, vis_data, interp_weights, tile_rows, facet_list, vis_count))
    gradient = gradient.transpose(2, 0, 3, 1, 4).reshape(CHANNELS, NY, NX)
    stepped = sky_image.astype(jnp.float32) - descent_step * gradient
    coarse = stepped
    clipped_sum = jnp.zeros_like(stepped)
    for level_index in range(LEVELS):
        smoother = smooth_both(coarse, 2 ** level_index)
        detail = coarse - smoother
        bound_now = wavelet_threshold[level_index][:, None, None]
        clipped_sum = clipped_sum + jnp.clip(detail, -bound_now, bound_now)
        coarse = smoother
    shrunk = stepped - clipped_sum
    blocks = shrunk.reshape(CHANNELS, NFY, FACET, NFX, FACET)
    grams = jnp.einsum('cyaxb,dyaxb->yxcd', blocks, blocks, precision=top_precision)
    offset = spectral_weight * (FACET * FACET)
    matrices = jax.vmap(jax.vmap(shrink_matrix, in_axes=(0, None)), in_axes=(0, None))(grams, offset)
    restored = jnp.einsum('cyaxb,yxcd->dyaxb', blocks, matrices, precision=top_precision)
    return restored.reshape(CHANNELS, NY, NX)
```

```python
import functools
import math

import jax
import jax.numpy as jnp
import ml_dtypes
import numpy as np
from jax import lax
from jax.experimental import pallas as pl
from jax.experimental.pallas import tpu as pltpu
from jax.sharding import PartitionSpec as P

MESH = pl.DeviceIdType.MESH
F32 = jnp.float32
BF16 = jnp.bfloat16
STEP = 2.0


def tables(length):
    positions = np.arange(length)
    angles = (positions[:, None] * positions[None, :] % length) * (2.0 * math.pi / length)
    cosine = (np.cos(angles) / math.sqrt(length)).astype(np.float32)
    sinus = (np.sin(angles) / math.sqrt(length)).astype(np.float32)
    whole = np.concatenate(
        [np.concatenate([cosine, -sinus], axis=1), np.concatenate([sinus, cosine], axis=1)], axis=0
    )
    high = whole.astype(ml_dtypes.bfloat16)
    low = (whole - high.astype(np.float32)).astype(ml_dtypes.bfloat16)
    return np.stack([high, low])


def dot(a, b):
    return jnp.dot(a, b, preferred_element_type=F32)


def dot_nt(a, b):
    return lax.dot_general(a, b, (((1,), (1,)), ((), ())), preferred_element_type=F32)


def dot_tn(a, b):
    return lax.dot_general(a, b, (((0,), (0,)), ((), ())), preferred_element_type=F32)


def split(values):
    high = values.astype(BF16)
    return high, (values - high.astype(F32)).astype(BF16)


def dot3(a, b):
    return dot(a[0], b[0]) + (dot(a[0], b[1]) + dot(a[1], b[0]))


def kernel(
    sizes,
    sky_hbm,
    vis_hbm,
    w_hbm,
    tiles_s,
    list_s,
    count_s,
    thr_s,
    mu_s,
    tab_hbm,
    out_ref,
    sky_v,
    vis_v,
    wv,
    tab,
    idx_send,
    idx_recv,
    spec,
    row_send,
    row_recv,
    con_buf,
    con_send,
    con_recv,
    inv_s,
    st_bf,
    edge_send,
    top_recv,
    bot_recv,
    vl,
    vr,
    ext,
    pa,
    pb,
    shr,
    shr_send,
    shr_recv,
    gpart,
    gtot,
    xs,
    local_sem,
    idx_ssem,
    idx_rsem,
    row_ssem,
    row_rsem,
    con_ssem,
    con_rsem,
    halo_ssem,
    halo_rsem,
    blk_ssem,
    blk_rsem,
):
    nfx, nfy, nblk, fpb, vt, nnz = sizes
    n_chan, size, _ = sky_v.shape
    slots = vt * nnz
    lanes = nfx * 2 * slots
    fy, fx, blk = lax.axis_index("fy"), lax.axis_index("fx"), lax.axis_index("blk")

    def along_fx(d):
        return (fy, lax.rem(fx + d, nfx), blk)

    up, down = lax.rem(fy + nfy - 1, nfy), lax.rem(fy + 1, nfy)
    left, right = lax.rem(fx + nfx - 1, nfx), lax.rem(fx + 1, nfx)
    mate = (fy, fx, 1 - blk)

    loads = []

    def load(src, dst):
        copy = pltpu.make_async_copy(src, dst, local_sem.at[len(loads)])
        copy.start()
        loads.append(copy)
        return copy

    tab_load = load(tab_hbm, tab)
    sky_load = load(sky_hbm, sky_v)
    vis_load = load(vis_hbm, vis_v)
    w_loads = [
        load(w_hbm.at[f, :, n], wv.at[f // 2, n, :, :, pl.ds((f % 2) * size, size)])
        for f in range(fpb)
        for n in range(nnz)
    ]

    barrier = pltpu.get_barrier_semaphore()
    others = [along_fx(d) for d in range(1, nfx)]
    others += [(up, fx, blk), (down, fx, blk), mate]
    others += [(r, c, blk) for r in (up, down) for c in (left, right)]
    for device in others:
        pl.semaphore_signal(barrier, inc=1, device_id=device, device_id_type=MESH)

    lane = lax.broadcasted_iota(jnp.int32, (1, lanes), 1)
    lane_a, lane_n = lane % vt, (lane // vt) % nnz
    lane_p, lane_j = (lane // slots) % 2, lane // (2 * slots)
    wanted = []
    for f in range(fpb):
        row = jnp.zeros((1, lanes), jnp.int32)
        for a in range(vt):
            for n in range(nnz):
                here = (lane_a == a) & (lane_n == n)
                row = jnp.where(here, tiles_s[(f * vt + a) * nnz + n], row)
        wanted.append(jnp.where(lane_j == fx, row + lane_p * size + 1, 0))
    for k in range(nfx):
        request = jnp.zeros((1, lanes), jnp.int32)
        place = fpb
        for f in range(fpb):
            hit = list_s[f] == k
            request = jnp.where(hit, wanted[f], request)
            place = jnp.where(hit, f, place)
        idx_send[k] = request
        inv_s[k] = place
    idx_recv[fx] = idx_send[fx]

    pl.semaphore_wait(barrier, len(others))

    order = sorted(range(1, nfx), key=lambda d: -min(d, nfx - d))

    def exchange(send, recv, ssem, rsem):
        copies = []
        for d in order:
            copy = pltpu.make_async_remote_copy(
                src_ref=send.at[lax.rem(fx + d, nfx)],
                dst_ref=recv.at[fx],
                send_sem=ssem.at[d],
                recv_sem=rsem.at[d],
                device_id=along_fx(d),
                device_id_type=MESH,
            )
            copy.start()
            copies.append(copy)
        return copies

    pending = exchange(idx_send, idx_recv, idx_ssem, idx_rsem)
    idx_copies = pending

    tab_load.wait()
    sky_load.wait()
    high = tab[0]
    left_table = jnp.concatenate([high[:size, :size], high[:size, size:]], axis=0)
    for c in range(n_chan):
        half = dot(left_table, sky_v[c]).astype(BF16)
        half = jnp.concatenate([half[:size], half[size:]], axis=1)
        full = dot(half, high).astype(BF16)
        spec[:size, c * size : (c + 1) * size] = full[:, :size]
        spec[size:, c * size : (c + 1) * size] = full[:, size:]

    for copy in idx_copies:
        copy.wait_recv()
    target = jnp.sum(idx_recv[...], axis=0)
    row_ids = lax.broadcasted_iota(jnp.int32, (2 * size, lanes), 0) + 1
    place_mat = jnp.where(row_ids == target, 1.0, 0.0).astype(BF16)
    group = 2 * slots
    for c in range(n_chan):
        picked = dot_tn(place_mat, spec[:, c * size : (c + 1) * size])
        row_send[:, c * group : (c + 1) * group, :] = picked.reshape(nfx, group, size).astype(BF16)
    row_recv[fx] = row_send[fx]
    row_copies = exchange(row_send, row_recv, row_ssem, row_rsem)

    rows_all = n_chan * 2 * slots
    n_vis = vt * size
    vis_load.wait()
    row_id = lax.broadcasted_iota(jnp.int32, (rows_all, n_vis), 0)
    vis_id = lax.broadcasted_iota(jnp.int32, (rows_all, n_vis), 1)
    live = (vis_id < count_s[0]) & (row_id % vt == vis_id // size)
    first_slot = (row_id // vt) % nnz == 0
    measured = []
    for c in range(n_chan):
        both = vis_v[c].astype(F32)
        for p in range(2):
            measured.append(jnp.broadcast_to(both[p : p + 1], (slots, n_vis)))
    measured = jnp.concatenate(measured, axis=0)
    con_buf[fpb] = jnp.zeros((rows_all, size), BF16)
    for copy in w_loads:
        copy.wait()
    for copy in row_copies:
        copy.wait_recv()

    sums = [None, None]
    for q in range(fpb // 2):
        x = jnp.concatenate([row_recv[list_s[2 * q]], row_recv[list_s[2 * q + 1]]], axis=1)
        for n in range(nnz):
            term = dot_nt(x, wv[q, n].reshape(n_vis, 2 * size))
            sums[n] = term if sums[n] is None else sums[n] + term
    mixed = jnp.where(first_slot, sums[0], sums[1])
    later = pltpu.roll(mixed, rows_all - vt, 0)
    earlier = pltpu.roll(mixed, vt, 0)
    predicted = mixed + jnp.where(first_slot, later, earlier)
    residual = jnp.where(live, predicted - measured, 0.0).astype(BF16)
    first_out = (lax.broadcasted_iota(jnp.int32, (rows_all, 2 * size), 0) // vt) % nnz == 0
    for q in range(fpb // 2):
        terms = [dot(residual, wv[q, n].reshape(n_vis, 2 * size)) for n in range(nnz)]
        out = jnp.where(first_out, terms[0], terms[1]).astype(BF16)
        con_buf[2 * q] = out[:, :size]
        con_buf[2 * q + 1] = out[:, size:]
    for k in range(nfx):
        con_send[k] = con_buf[inv_s[k]]
    con_recv[fx] = con_send[fx]
    con_copies = exchange(con_send, con_recv, con_ssem, con_rsem)

    def flipped(table):
        return jnp.concatenate(
            [
                jnp.concatenate([table[:size, :size], table[size:, :size]], axis=1),
                jnp.concatenate([table[:size, size:], table[size:, size:]], axis=1),
            ],
            axis=0,
        )

    for copy in con_copies:
        copy.wait_recv()
    right_back = (flipped(tab[0]), flipped(tab[1]))
    left_back = (tab[0, :size, :], tab[1, :size, :])
    edge = jnp.zeros((size, size), F32)
    lane_c = lax.broadcasted_iota(jnp.int32, (size, size), 1) // 32
    for c in range(n_chan):
        incoming = con_recv[:, c * group : (c + 1) * group, :].reshape(nfx * group, size)
        own = dot(place_mat, incoming)
        own = jnp.concatenate([own[:size], own[size:]], axis=1)
        half = dot3(split(own), right_back)
        half = jnp.concatenate([half[:, :size], half[:, size:]], axis=0)
        grad = dot3(left_back, split(half))
        stepped = sky_v[c].astype(F32) - STEP * grad
        ext[c, 0, 24 : 24 + size, :] = stepped
        shr[c] = stepped
        st_bf[c] = stepped.astype(BF16)
        edge = jnp.where(lane_c == c, pltpu.roll(stepped, 16 + 32 * c, 1), edge)
    edge_send[...] = edge.astype(BF16)

    last = size - 16
    halo = [
        (st_bf.at[:, pl.ds(0, 16), :], bot_recv, (up, fx, blk)),
        (st_bf.at[:, pl.ds(last, 16), :], top_recv, (down, fx, blk)),
        (edge_send, vr.at[pl.ds(16, size), :], (fy, left, blk)),
        (edge_send, vl.at[pl.ds(16, size), :], (fy, right, blk)),
        (edge_send.at[pl.ds(0, 16), :], vr.at[pl.ds(16 + size, 16), :], (up, left, blk)),
        (edge_send.at[pl.ds(0, 16), :], vl.at[pl.ds(16 + size, 16), :], (up, right, blk)),
        (edge_send.at[pl.ds(last, 16), :], vr.at[pl.ds(0, 16), :], (down, left, blk)),
        (edge_send.at[pl.ds(last, 16), :], vl.at[pl.ds(0, 16), :], (down, right, blk)),
    ]
    halo_copies = []
    for h in (4, 5, 6, 7, 2, 3, 0, 1):
        src, dst, device = halo[h]
        copy = pltpu.make_async_remote_copy(
            src_ref=src,
            dst_ref=dst,
            send_sem=halo_ssem.at[h],
            recv_sem=halo_rsem.at[h],
            device_id=device,
            device_id_type=MESH,
        )
        copy.start()
        halo_copies.append(copy)

    tall = size + 32
    in_top, in_bottom = fy > 0, fy < nfy - 1
    in_left, in_right = fx > 0, fx < nfx - 1
    lane_id = lax.broadcasted_iota(jnp.int32, (1, size), 1)
    side_live = ((lane_id < 64) & in_right) | ((lane_id >= 64) & in_left)
    row_tall = lax.broadcasted_iota(jnp.int32, (tall, 1), 0)
    rows_live = ((row_tall >= 16) | in_top) & ((row_tall < 16 + size) | in_bottom)
    wide_live = rows_live & side_live

    for copy in halo_copies:
        copy.wait_recv()
    from_left = vl[...].astype(F32)
    from_right = vr[...].astype(F32)
    zeros8 = jnp.zeros((8, size), F32)
    for c in range(n_chan):
        ext[c, 0, 8:24, :] = jnp.where(in_top, top_recv[c].astype(F32), 0.0)
        ext[c, 0, 24 + size : 40 + size, :] = jnp.where(in_bottom, bot_recv[c].astype(F32), 0.0)
        r = pltpu.roll(from_right, (size - (32 * c + 16)) % size, 1)
        l = pltpu.roll(from_left, (size - 16 - 32 * c) % size, 1)
        side = jnp.where(lane_id < 16, r, jnp.where(lane_id >= size - 16, l, 0.0))
        ext[c, 1, 8 : 8 + tall, :] = jnp.where(wide_live, side, 0.0)
        for t in range(2):
            ext[c, t, 0:8, :] = zeros8
            ext[c, t, 8 + tall : 16 + tall, :] = zeros8
    for buf in (pa, pb):
        for t in range(2):
            buf[t, 0:8, :] = zeros8
            buf[t, 8 + tall : 16 + tall, :] = zeros8

    spans = [(8, 8 + tall, 32), (8, 8 + tall, 32), (16, tall, 48), (24, 24 + size, 32)]
    blk_copies = []
    for c in range(n_chan):
        source = ext.at[c]
        for level in range(len(spans)):
            s = 2**level
            low, top, chunk = spans[level]
            final = level == len(spans) - 1
            dest = None if final else (pa, pb)[level % 2]
            bound = thr_s[level, c]
            for at in range(low, top, chunk):
                tiles = []
                for t in range(2):
                    tiles.append(
                        (
                            source[t, at - s : at - s + chunk, :]
                            + 2.0 * source[t, at : at + chunk, :]
                            + source[t, at + s : at + s + chunk, :]
                        )
                        * 0.25
                    )
                rr = [pltpu.roll(v, s, 1) for v in tiles]
                ll = [pltpu.roll(v, size - s, 1) for v in tiles]
                lo_lane, hi_lane = lane_id < s, lane_id >= size - s
                smooth = (
                    jnp.where(lo_lane, rr[1], rr[0])
                    + 2.0 * tiles[0]
                    + jnp.where(hi_lane, ll[1], ll[0])
                ) * 0.25
                if not final:
                    side = (
                        jnp.where(lo_lane, rr[0], rr[1])
                        + 2.0 * tiles[1]
                        + jnp.where(hi_lane, ll[0], ll[1])
                    ) * 0.25
                    inside = rows_live[at - 8 : at - 8 + chunk]
                    if at < 24 or at + chunk > 24 + size:
                        smooth = jnp.where(inside, smooth, 0.0)
                        side = jnp.where(inside & side_live, side, 0.0)
                    else:
                        side = jnp.where(side_live, side, 0.0)
                    dest[0, at : at + chunk, :] = smooth
                    dest[1, at : at + chunk, :] = side
                first, stop = max(at, 24), min(at + chunk, 24 + size)
                detail = source[0, first:stop, :] - smooth[first - at : stop - at]
                own_rows = slice(first - 24, stop - 24)
                shr[c, own_rows, :] = shr[c, own_rows, :] - jnp.clip(detail, -bound, bound)
            source = dest
        shr_send[c] = shr[c].astype(BF16)
        copy = pltpu.make_async_remote_copy(
            src_ref=shr_send.at[c],
            dst_ref=shr_recv.at[c],
            send_sem=blk_ssem.at[c],
            recv_sem=blk_rsem.at[c],
            device_id=mate,
            device_id_type=MESH,
        )
        copy.start()
        blk_copies.append(copy)

    total = 2 * n_chan
    chunk = 16

    def products(pairs, first):
        def step(i, sums):
            rows = pl.ds(pl.multiple_of(i * chunk, chunk), chunk)
            vals = [shr[c, rows, :] for c in range(n_chan)]
            if not first:
                vals += [shr_recv[c, rows, :].astype(F32) for c in range(n_chan)]
            news = []
            for k, (a, b) in enumerate(pairs):
                prod = vals[a] * vals[b]
                news.append(sums[k] + (prod[:8] + prod[8:]))
            return tuple(news)

        start = tuple(jnp.zeros((8, size), F32) for _ in pairs)
        sums = lax.fori_loop(0, size // chunk, step, start)
        for (a, b), value in zip(pairs, sums):
            value = jnp.sum(value, axis=0, keepdims=True)
            gpart[a * total + b : a * total + b + 1, :] = value
            if a != b:
                gpart[b * total + a : b * total + a + 1, :] = value

    everyone = [(a, b) for a in range(total) for b in range(a, total)]
    products([(a, b) for a, b in everyone if b < n_chan], True)
    for copy in blk_copies:
        copy.wait_recv()
    products([(a, b) for a, b in everyone if b >= n_chan], False)
    gtot[...] = jnp.broadcast_to(jnp.sum(gpart[...], axis=1, keepdims=True), gtot.shape)

    mu = mu_s[0] * float(size * size)
    mat = {}
    for a, b in everyone:
        value = jnp.broadcast_to(gtot[a * total + b : a * total + b + 1, :], (total, size))
        mat[a, b] = value + mu if a == b else value
    rhs = [gtot[c * total : (c + 1) * total, :] for c in range(total)]
    inverse = [None] * total
    for k in range(total):
        inverse[k] = 1.0 / mat[k, k]
        for i in range(k + 1, total):
            factor = mat[k, i] * inverse[k]
            for j in range(i, total):
                mat[i, j] = mat[i, j] - factor * mat[k, j]
            rhs[i] = rhs[i] - factor * rhs[k]
    solved = [None] * total
    for k in range(total - 1, -1, -1):
        value = rhs[k]
        for i in range(k + 1, total):
            value = value - mat[k, i] * solved[i]
        solved[k] = value * inverse[k]
        xs[k * total : (k + 1) * total, :] = solved[k]

    coeffs = [
        [jnp.broadcast_to(xs[c * total + d : c * total + d + 1, :], (8, size)) for c in range(total)]
        for d in range(n_chan)
    ]

    def finish(i, carry):
        rows = pl.ds(pl.multiple_of(i * chunk, chunk), chunk)
        vals = [shr[c, rows, :] for c in range(n_chan)]
        vals += [shr_recv[c, rows, :].astype(F32) for c in range(n_chan)]
        for d in range(n_chan):
            for h in range(2):
                value = coeffs[d][0] * vals[0][h * 8 : h * 8 + 8]
                for c in range(1, total):
                    value = value + coeffs[d][c] * vals[c][h * 8 : h * 8 + 8]
                out_ref[d, pl.ds(pl.multiple_of(i * chunk + h * 8, 8), 8), :] = value
        return carry

    lax.fori_loop(0, size // chunk, finish, 0)

    for copy in idx_copies + row_copies + con_copies + halo_copies + blk_copies:
        copy.wait_send()


def body(sizes, sky, vis, weights, tiles, lists, count, threshold, weight):
    nfx, nfy, nblk, fpb, vt, nnz = sizes
    n_chan, size, _ = sky.shape
    rows = n_chan * 2 * vt * nnz
    lanes = nfx * 2 * vt * nnz
    hbm = pl.BlockSpec(memory_space=pl.ANY)
    smem = pl.BlockSpec(memory_space=pltpu.SMEM)
    tall = size + 48
    sem = pltpu.SemaphoreType.DMA
    return pl.pallas_call(
        functools.partial(kernel, sizes),
        out_shape=jax.ShapeDtypeStruct((n_chan, size, size), F32),
        in_specs=[hbm, hbm, hbm, smem, smem, smem, smem, smem, hbm],
        out_specs=pl.BlockSpec(memory_space=pltpu.VMEM),
        scratch_shapes=[
            pltpu.VMEM((n_chan, size, size), BF16),
            pltpu.VMEM((n_chan, 2, vt * size), BF16),
            pltpu.VMEM((fpb // 2, nnz, vt, size, 2 * size), BF16),
            pltpu.VMEM((2, 2 * size, 2 * size), BF16),
            pltpu.VMEM((nfx, 1, lanes), jnp.int32),
            pltpu.VMEM((nfx, 1, lanes), jnp.int32),
            pltpu.VMEM((2 * size, n_chan * size), BF16),
            pltpu.VMEM((nfx, rows, size), BF16),
            pltpu.VMEM((nfx, rows, size), BF16),
            pltpu.VMEM((fpb + 1, rows, size), BF16),
            pltpu.VMEM((nfx, rows, size), BF16),
            pltpu.VMEM((nfx, rows, size), BF16),
            pltpu.SMEM((nfx,), jnp.int32),
            pltpu.VMEM((n_chan, size, size), BF16),
            pltpu.VMEM((size, size), BF16),
            pltpu.VMEM((n_chan, 16, size), BF16),
            pltpu.VMEM((n_chan, 16, size), BF16),
            pltpu.VMEM((size + 32, size), BF16),
            pltpu.VMEM((size + 32, size), BF16),
            pltpu.VMEM((n_chan, 2, tall, size), F32),
            pltpu.VMEM((2, tall, size), F32),
            pltpu.VMEM((2, tall, size), F32),
            pltpu.VMEM((n_chan, size, size), F32),
            pltpu.VMEM((n_chan, size, size), BF16),
            pltpu.VMEM((n_chan, size, size), BF16),
            pltpu.VMEM((4 * n_chan * n_chan, size), F32),
            pltpu.VMEM((4 * n_chan * n_chan, size), F32),
            pltpu.VMEM((4 * n_chan * n_chan, size), F32),
            sem((3 + fpb * nnz,)),
            sem((nfx,)),
            sem((nfx,)),
            sem((nfx,)),
            sem((nfx,)),
            sem((nfx,)),
            sem((nfx,)),
            sem((8,)),
            sem((8,)),
            sem((n_chan,)),
            sem((n_chan,)),
        ],
        compiler_params=pltpu.CompilerParams(collective_id=0, has_side_effects=True),
    )(
        sky,
        vis[0, 0],
        weights[0, 0],
        tiles.reshape(-1),
        lists.reshape(-1),
        count.reshape(-1),
        threshold,
        weight.reshape(1),
        jnp.asarray(tables(size)),
    )


def solution(mesh):
    in_specs = (
        P("blk", "fy", "fx"),
        P("fy", "fx", "blk", None, None),
        P("fy", "fx", None, None, None, None, None),
        P("fy", "fx", None, None, None),
        P("fy", "fx", None),
        P("fy", "fx"),
        P(None, "blk"),
        P(),
    )

    def step(*args):
        fpb, vt, nnz = args[3].shape[2:]
        sizes = (mesh.shape["fx"], mesh.shape["fy"], mesh.shape["blk"], fpb, vt, nnz)
        return body(sizes, *args)

    return jax.shard_map(
        step, mesh=mesh, in_specs=in_specs, out_specs=P("blk", "fy", "fx"), check_vma=False
    )
```

```python
import functools
import math

import jax
import jax.numpy as jnp
import ml_dtypes
import numpy as np
from jax import lax
from jax.experimental import pallas as pl
from jax.experimental.pallas import tpu as pltpu
from jax.sharding import PartitionSpec as P

MESH = pl.DeviceIdType.MESH
F32 = jnp.float32
BF16 = jnp.bfloat16
STEP = 2.0


def tables(length):
    positions = np.arange(length)
    angles = (positions[:, None] * positions[None, :] % length) * (2.0 * math.pi / length)
    cosine = (np.cos(angles) / math.sqrt(length)).astype(np.float32)
    sinus = (np.sin(angles) / math.sqrt(length)).astype(np.float32)
    whole = np.concatenate(
        [np.concatenate([cosine, -sinus], axis=1), np.concatenate([sinus, cosine], axis=1)], axis=0
    )
    high = whole.astype(ml_dtypes.bfloat16)
    low = (whole - high.astype(np.float32)).astype(ml_dtypes.bfloat16)
    return np.stack([high, low])


def dot(a, b):
    return jnp.dot(a, b, preferred_element_type=F32)


def dot_nt(a, b):
    return lax.dot_general(a, b, (((1,), (1,)), ((), ())), preferred_element_type=F32)


def dot_tn(a, b):
    return lax.dot_general(a, b, (((0,), (0,)), ((), ())), preferred_element_type=F32)


def split(values):
    high = values.astype(BF16)
    return high, (values - high.astype(F32)).astype(BF16)


def dot3(a, b):
    return dot(a[0], b[0]) + (dot(a[0], b[1]) + dot(a[1], b[0]))


def pinned(array):
    return pltpu.with_memory_space_constraint(array, pltpu.HBM)


def kernel(
    sizes,
    sky_hbm,
    vis_hbm,
    w_hbm,
    tiles_hbm,
    list_hbm,
    count_s,
    thr_hbm,
    tab_hbm,
    shr,
    other,
    tiles_s,
    list_s,
    thr_s,
    sky_v,
    vis_v,
    wv,
    tab,
    idx_send,
    idx_recv,
    spec,
    row_send,
    row_recv0,
    row_recv1,
    con_buf,
    con_send,
    con_recv,
    inv_s,
    st_bf,
    edge_send,
    top_recv,
    bot_recv,
    vl,
    vr,
    ext,
    pa,
    pb,
    shr_send,
    shr_recv,
    local_sem,
    idx_ssem,
    idx_rsem,
    row_ssem,
    row_rsem,
    con_ssem,
    con_rsem,
    halo_ssem,
    halo_rsem,
    blk_ssem,
    blk_rsem,
):
    nfx, nfy, nblk, fpb, vt, nnz, halves = sizes
    n_chan, size, _ = sky_v.shape
    per = n_chan // halves
    row_recv = (row_recv0, row_recv1)
    slots = vt * nnz
    lanes = nfx * 2 * slots
    fy, fx, blk = lax.axis_index("fy"), lax.axis_index("fx"), lax.axis_index("blk")

    def along_fx(d):
        return (fy, lax.rem(fx + d, nfx), blk)

    up, down = lax.rem(fy + nfy - 1, nfy), lax.rem(fy + 1, nfy)
    left, right = lax.rem(fx + nfx - 1, nfx), lax.rem(fx + 1, nfx)
    mate = (fy, fx, 1 - blk)

    loads = []

    def load(src, dst):
        copy = pltpu.make_async_copy(src, dst, local_sem.at[len(loads)])
        copy.start()
        loads.append(copy)
        return copy

    barrier = pltpu.get_barrier_semaphore()
    others = [along_fx(d) for d in range(1, nfx)]
    others += [(up, fx, blk), (down, fx, blk), mate]
    others += [(r, c, blk) for r in (up, down) for c in (left, right)]
    for device in others:
        pl.semaphore_signal(barrier, inc=1, device_id=device, device_id_type=MESH)

    small_loads = [
        load(tiles_hbm, tiles_s),
        load(list_hbm, list_s),
        load(thr_hbm, thr_s),
    ]
    tab_load = load(tab_hbm, tab)
    sky_load = load(sky_hbm, sky_v)
    vis_load = load(vis_hbm, vis_v)
    w_loads = [
        load(w_hbm.at[f, :, n], wv.at[f // 2, n, :, :, pl.ds((f % 2) * size, size)])
        for f in range(fpb)
        for n in range(nnz)
    ]

    for copy in small_loads:
        copy.wait()
    lane = lax.broadcasted_iota(jnp.int32, (1, lanes), 1)
    lane_a, lane_n = lane % vt, (lane // vt) % nnz
    lane_p, lane_j = (lane // slots) % 2, lane // (2 * slots)
    wanted = []
    for f in range(fpb):
        row = jnp.zeros((1, lanes), jnp.int32)
        for a in range(vt):
            for n in range(nnz):
                here = (lane_a == a) & (lane_n == n)
                row = jnp.where(here, tiles_s[a, n, f], row)
        wanted.append(jnp.where(lane_j == fx, row + lane_p * size + 1, 0))
    for k in range(nfx):
        request = jnp.zeros((1, lanes), jnp.int32)
        place = fpb
        for f in range(fpb):
            hit = list_s[f] == k
            request = jnp.where(hit, wanted[f], request)
            place = jnp.where(hit, f, place)
        idx_send[k] = request
        inv_s[k] = place
    idx_recv[fx] = idx_send[fx]

    pl.semaphore_wait(barrier, len(others))

    order = sorted(range(1, nfx), key=lambda d: -min(d, nfx - d))

    def exchange(send, recv, ssem, rsem):
        copies = []
        for d in order:
            copy = pltpu.make_async_remote_copy(
                src_ref=send.at[lax.rem(fx + d, nfx)],
                dst_ref=recv.at[fx],
                send_sem=ssem.at[d],
                recv_sem=rsem.at[d],
                device_id=along_fx(d),
                device_id_type=MESH,
            )
            copy.start()
            copies.append(copy)
        return copies

    idx_copies = exchange(idx_send, idx_recv, idx_ssem, idx_rsem)

    tab_load.wait()
    sky_load.wait()
    high = tab[0]
    left_table = jnp.concatenate([high[:size, :size], high[:size, size:]], axis=0)
    for c in range(n_chan):
        half = dot(left_table, sky_v[c]).astype(BF16)
        half = jnp.concatenate([half[:size], half[size:]], axis=1)
        full = dot(half, high).astype(BF16)
        spec[:size, c * size : (c + 1) * size] = full[:, :size]
        spec[size:, c * size : (c + 1) * size] = full[:, size:]

    for copy in idx_copies:
        copy.wait_recv()
    target = jnp.sum(idx_recv[...], axis=0)
    row_ids = lax.broadcasted_iota(jnp.int32, (2 * size, lanes), 0) + 1
    place_mat = jnp.where(row_ids == target, 1.0, 0.0).astype(BF16)
    group = 2 * slots
    row_copies = []
    for h in range(halves):
        span = slice(h * per * size, (h + 1) * per * size)
        picked = dot_tn(place_mat, spec[:, span]).astype(BF16)
        for c in range(per):
            row_send[h, :, c * group : (c + 1) * group, :] = picked[
                :, c * size : (c + 1) * size
            ].reshape(nfx, group, size)
        row_recv[h][fx] = row_send[h, fx]
        row_copies.append(
            exchange(row_send.at[h], row_recv[h], row_ssem.at[h], row_rsem.at[h])
        )

    rows_all = per * group
    n_vis = vt * size
    vis_load.wait()
    row_id = lax.broadcasted_iota(jnp.int32, (rows_all, n_vis), 0)
    vis_id = lax.broadcasted_iota(jnp.int32, (rows_all, n_vis), 1)
    live = (vis_id < count_s[0]) & (row_id % vt == vis_id // size)
    first_slot = (row_id // vt) % nnz == 0
    first_out = (lax.broadcasted_iota(jnp.int32, (rows_all, 2 * size), 0) // vt) % nnz == 0
    for h in range(halves):
        con_buf[h, fpb] = jnp.zeros((rows_all, size), BF16)
    for copy in w_loads:
        copy.wait()

    con_copies = []
    for h in range(halves):
        for copy in row_copies[h]:
            copy.wait_recv()
        measured = []
        for c in range(per):
            both = vis_v[h * per + c].astype(F32)
            for p in range(2):
                measured.append(jnp.broadcast_to(both[p : p + 1], (slots, n_vis)))
        measured = jnp.concatenate(measured, axis=0)
        sums = [None, None]
        for q in range(fpb // 2):
            x = jnp.concatenate(
                [row_recv[h][list_s[2 * q]], row_recv[h][list_s[2 * q + 1]]], axis=1
            )
            for n in range(nnz):
                term = dot_nt(x, wv[q, n].reshape(n_vis, 2 * size))
                sums[n] = term if sums[n] is None else sums[n] + term
        mixed = jnp.where(first_slot, sums[0], sums[1])
        later = pltpu.roll(mixed, rows_all - vt, 0)
        earlier = pltpu.roll(mixed, vt, 0)
        predicted = mixed + jnp.where(first_slot, later, earlier)
        residual = jnp.where(live, predicted - measured, 0.0).astype(BF16)
        for q in range(fpb // 2):
            terms = [dot(residual, wv[q, n].reshape(n_vis, 2 * size)) for n in range(nnz)]
            out = jnp.where(first_out, terms[0], terms[1]).astype(BF16)
            con_buf[h, 2 * q] = out[:, :size]
            con_buf[h, 2 * q + 1] = out[:, size:]
        for k in range(nfx):
            con_send[h, k] = con_buf[h, inv_s[k]]
        con_recv[h, fx] = con_send[h, fx]
        con_copies.append(
            exchange(con_send.at[h], con_recv.at[h], con_ssem.at[h], con_rsem.at[h])
        )

    def flipped(table):
        return jnp.concatenate(
            [
                jnp.concatenate([table[:size, :size], table[size:, :size]], axis=1),
                jnp.concatenate([table[:size, size:], table[size:, size:]], axis=1),
            ],
            axis=0,
        )

    right_back = (flipped(tab[0]), flipped(tab[1]))
    left_back = (tab[0, :size, :], tab[1, :size, :])
    lane_id = lax.broadcasted_iota(jnp.int32, (1, size), 1)
    mid = size // 2
    halo_copies = []
    for h in range(halves):
        for copy in con_copies[h]:
            copy.wait_recv()
        incoming = jnp.concatenate(
            [
                con_recv[h, :, c * group : (c + 1) * group, :].reshape(nfx * group, size)
                for c in range(per)
            ],
            axis=1,
        )
        own = dot(place_mat, incoming)
        own = jnp.concatenate(
            [
                jnp.concatenate(
                    [own[:size, c * size : (c + 1) * size], own[size:, c * size : (c + 1) * size]],
                    axis=1,
                )
                for c in range(per)
            ],
            axis=0,
        )
        half = dot3(split(own), right_back)
        half = jnp.concatenate(
            [
                jnp.concatenate(
                    [half[c * size : (c + 1) * size, :size], half[c * size : (c + 1) * size, size:]],
                    axis=0,
                )
                for c in range(per)
            ],
            axis=1,
        )
        grad = dot3(left_back, split(half))
        edge = jnp.zeros((mid, size), F32)
        for c in range(per):
            stepped = sky_v[h * per + c].astype(F32) - STEP * grad[:, c * size : (c + 1) * size]
            ext[h * per + c, 0, 24 : 24 + size, :] = stepped
            shr[h * per + c] = stepped
            st_bf[h, c] = stepped.astype(BF16)
            for fold in range(2):
                at = fold * mid + 32 * c
                part = pltpu.roll(stepped[fold * mid : (fold + 1) * mid], (16 + at) % size, 1)
                edge = jnp.where((lane_id >= at) & (lane_id < at + 32), part, edge)
        edge_send[h] = edge.astype(BF16)

        first, last = pl.ds(0, 16), pl.ds(mid - 16, 16)
        main, low = pl.ds(16, mid), pl.ds(16 + mid, 16)
        halo = [
            (edge_send.at[h, first], vr.at[h, low], (up, left, blk)),
            (edge_send.at[h, first], vl.at[h, low], (up, right, blk)),
            (edge_send.at[h, last], vr.at[h, first], (down, left, blk)),
            (edge_send.at[h, last], vl.at[h, first], (down, right, blk)),
            (edge_send.at[h], vr.at[h, main], (fy, left, blk)),
            (edge_send.at[h], vl.at[h, main], (fy, right, blk)),
            (st_bf.at[h, :, pl.ds(0, 16), :], bot_recv.at[h], (up, fx, blk)),
            (st_bf.at[h, :, pl.ds(size - 16, 16), :], top_recv.at[h], (down, fx, blk)),
        ]
        copies = []
        for k, (src, dst, device) in enumerate(halo):
            copy = pltpu.make_async_remote_copy(
                src_ref=src,
                dst_ref=dst,
                send_sem=halo_ssem.at[h, k],
                recv_sem=halo_rsem.at[h, k],
                device_id=device,
                device_id_type=MESH,
            )
            copy.start()
            copies.append(copy)
        halo_copies.append(copies)

    tall = size + 32
    in_top, in_bottom = fy > 0, fy < nfy - 1
    in_left, in_right = fx > 0, fx < nfx - 1
    side_live = ((lane_id < 64) & in_right) | ((lane_id >= 64) & in_left)
    row_tall = lax.broadcasted_iota(jnp.int32, (tall, 1), 0)
    rows_live = ((row_tall >= 16) | in_top) & ((row_tall < 16 + size) | in_bottom)
    zeros8 = jnp.zeros((8, size), F32)
    for buf in [pa, pb] + [ext.at[c] for c in range(n_chan)]:
        for t in range(2):
            buf[t, 0:8, :] = zeros8
            buf[t, 8 + tall : 16 + tall, :] = zeros8
    spans = [(8, 8 + tall, 32), (8, 8 + tall, 32), (16, tall, 48), (24, 24 + size, 32)]
    pieces = [(0, 0, 16, 1), (16, 16, mid, 0), (16 + mid, 16, mid, 1), (16 + size, 16 + mid, 16, 0)]

    blk_copies = []
    for h in range(halves):
        for copy in halo_copies[h]:
            copy.wait_recv()
        from_left = vl[h].astype(F32)
        from_right = vr[h].astype(F32)
        for q in range(per):
            c = h * per + q
            ext[c, 0, 8:24, :] = jnp.where(in_top, top_recv[h, q].astype(F32), 0.0)
            ext[c, 0, 24 + size : 40 + size, :] = jnp.where(
                in_bottom, bot_recv[h, q].astype(F32), 0.0
            )
            for to, start, count, fold in pieces:
                at = fold * mid + 32 * q
                r = pltpu.roll(from_right[start : start + count], (2 * size - at - 16) % size, 1)
                l = pltpu.roll(from_left[start : start + count], (2 * size - at - 16) % size, 1)
                side = jnp.where(lane_id < 16, r, jnp.where(lane_id >= size - 16, l, 0.0))
                side = jnp.where(rows_live[to : to + count] & side_live, side, 0.0)
                ext[c, 1, 8 + to : 8 + to + count, :] = side
        for q in range(per):
            c = h * per + q
            source = ext.at[c]
            for level in range(len(spans)):
                s = 2**level
                low, top, chunk = spans[level]
                final = level == len(spans) - 1
                dest = None if final else (pa, pb)[level % 2]
                bound = thr_s[level, c]
                for at in range(low, top, chunk):
                    tiles = []
                    for t in range(2):
                        tiles.append(
                            (
                                source[t, at - s : at - s + chunk, :]
                                + 2.0 * source[t, at : at + chunk, :]
                                + source[t, at + s : at + s + chunk, :]
                            )
                            * 0.25
                        )
                    rr = [pltpu.roll(v, s, 1) for v in tiles]
                    ll = [pltpu.roll(v, size - s, 1) for v in tiles]
                    lo_lane, hi_lane = lane_id < s, lane_id >= size - s
                    smooth = (
                        jnp.where(lo_lane, rr[1], rr[0])
                        + 2.0 * tiles[0]
                        + jnp.where(hi_lane, ll[1], ll[0])
                    ) * 0.25
                    if not final:
                        side = (
                            jnp.where(lo_lane, rr[0], rr[1])
                            + 2.0 * tiles[1]
                            + jnp.where(hi_lane, ll[0], ll[1])
                        ) * 0.25
                        inside = rows_live[at - 8 : at - 8 + chunk]
                        if at < 24 or at + chunk > 24 + size:
                            smooth = jnp.where(inside, smooth, 0.0)
                            side = jnp.where(inside & side_live, side, 0.0)
                        else:
                            side = jnp.where(side_live, side, 0.0)
                        dest[0, at : at + chunk, :] = smooth
                        dest[1, at : at + chunk, :] = side
                    first, stop = max(at, 24), min(at + chunk, 24 + size)
                    detail = source[0, first:stop, :] - smooth[first - at : stop - at]
                    own_rows = slice(first - 24, stop - 24)
                    shr[c, own_rows, :] = shr[c, own_rows, :] - jnp.clip(detail, -bound, bound)
                source = dest
            shr_send[c] = shr[c].astype(BF16)
            copy = pltpu.make_async_remote_copy(
                src_ref=shr_send.at[c],
                dst_ref=shr_recv.at[c],
                send_sem=blk_ssem.at[c],
                recv_sem=blk_rsem.at[c],
                device_id=mate,
                device_id_type=MESH,
            )
            copy.start()
            blk_copies.append(copy)

    for c, copy in enumerate(blk_copies):
        copy.wait_recv()
        other[c] = shr_recv[c]

    for copies in [idx_copies] + row_copies + con_copies + halo_copies + [blk_copies]:
        for copy in copies:
            copy.wait_send()


def last_kernel(shr, other, mu_s, out_ref, gpart, gtot, xs):
    n_chan, size, _ = shr.shape
    total = 2 * n_chan
    chunk = 16
    pairs = [(a, b) for a in range(total) for b in range(a, total)]

    def step(i, sums):
        rows = pl.ds(pl.multiple_of(i * chunk, chunk), chunk)
        vals = [shr[c, rows, :] for c in range(n_chan)]
        vals += [other[c, rows, :].astype(F32) for c in range(n_chan)]
        news = []
        for k, (a, b) in enumerate(pairs):
            prod = vals[a] * vals[b]
            news.append(sums[k] + (prod[:8] + prod[8:]))
        return tuple(news)

    sums = lax.fori_loop(
        0, size // chunk, step, tuple(jnp.zeros((8, size), F32) for _ in pairs)
    )
    for (a, b), value in zip(pairs, sums):
        value = jnp.sum(value, axis=0, keepdims=True)
        gpart[a * total + b : a * total + b + 1, :] = value
        if a != b:
            gpart[b * total + a : b * total + a + 1, :] = value
    gtot[...] = jnp.broadcast_to(jnp.sum(gpart[...], axis=1, keepdims=True), gtot.shape)

    mu = mu_s[0] * float(size * size)
    mat = {}
    for a, b in pairs:
        value = jnp.broadcast_to(gtot[a * total + b : a * total + b + 1, :], (total, size))
        mat[a, b] = value + mu if a == b else value
    rhs = [gtot[c * total : (c + 1) * total, :] for c in range(total)]
    inverse = [None] * total
    for k in range(total):
        inverse[k] = 1.0 / mat[k, k]
        for i in range(k + 1, total):
            factor = mat[k, i] * inverse[k]
            for j in range(i, total):
                mat[i, j] = mat[i, j] - factor * mat[k, j]
            rhs[i] = rhs[i] - factor * rhs[k]
    solved = [None] * total
    for k in range(total - 1, -1, -1):
        value = rhs[k]
        for i in range(k + 1, total):
            value = value - mat[k, i] * solved[i]
        solved[k] = value * inverse[k]
        xs[k * total : (k + 1) * total, :] = solved[k]

    coeffs = [
        [jnp.broadcast_to(xs[c * total + d : c * total + d + 1, :], (8, size)) for c in range(total)]
        for d in range(n_chan)
    ]

    def finish(i, carry):
        rows = pl.ds(pl.multiple_of(i * chunk, chunk), chunk)
        vals = [shr[c, rows, :] for c in range(n_chan)]
        vals += [other[c, rows, :].astype(F32) for c in range(n_chan)]
        for d in range(n_chan):
            for h in range(2):
                value = coeffs[d][0] * vals[0][h * 8 : h * 8 + 8]
                for c in range(1, total):
                    value = value + coeffs[d][c] * vals[c][h * 8 : h * 8 + 8]
                out_ref[d, pl.ds(pl.multiple_of(i * chunk + h * 8, 8), 8), :] = value
        return carry

    lax.fori_loop(0, size // chunk, finish, 0)


def body(sizes, sky, vis, weights, tiles, lists, count, threshold, weight):
    nfx, nfy, nblk, fpb, vt, nnz, halves = sizes
    n_chan, size, _ = sky.shape
    per = n_chan // halves
    rows = per * 2 * vt * nnz
    lanes = nfx * 2 * vt * nnz
    hbm = pl.BlockSpec(memory_space=pltpu.HBM)
    smem = pl.BlockSpec(memory_space=pltpu.SMEM)
    vmem = pl.BlockSpec(memory_space=pltpu.VMEM)
    tall = size + 48
    sem = pltpu.SemaphoreType.DMA
    shr, other = pl.pallas_call(
        functools.partial(kernel, sizes),
        out_shape=[
            jax.ShapeDtypeStruct((n_chan, size, size), F32),
            jax.ShapeDtypeStruct((n_chan, size, size), BF16),
        ],
        in_specs=[hbm] * 5 + [smem, hbm, hbm],
        out_specs=[vmem, vmem],
        scratch_shapes=[
            pltpu.SMEM((vt, nnz, fpb), jnp.int32),
            pltpu.SMEM((fpb,), jnp.int32),
            pltpu.SMEM(threshold.shape, F32),
            pltpu.VMEM((n_chan, size, size), BF16),
            pltpu.VMEM((n_chan, 2, vt * size), BF16),
            pltpu.VMEM((fpb // 2, nnz, vt, size, 2 * size), BF16),
            pltpu.VMEM((2, 2 * size, 2 * size), BF16),
            pltpu.VMEM((nfx, 1, lanes), jnp.int32),
            pltpu.VMEM((nfx, 1, lanes), jnp.int32),
            pltpu.VMEM((2 * size, n_chan * size), BF16),
            pltpu.VMEM((halves, nfx, rows, size), BF16),
            pltpu.VMEM((nfx, rows, size), BF16),
            pltpu.VMEM((nfx, rows, size), BF16),
            pltpu.VMEM((halves, fpb + 1, rows, size), BF16),
            pltpu.VMEM((halves, nfx, rows, size), BF16),
            pltpu.VMEM((halves, nfx, rows, size), BF16),
            pltpu.SMEM((nfx,), jnp.int32),
            pltpu.VMEM((halves, per, size, size), BF16),
            pltpu.VMEM((halves, size // 2, size), BF16),
            pltpu.VMEM((halves, per, 16, size), BF16),
            pltpu.VMEM((halves, per, 16, size), BF16),
            pltpu.VMEM((halves, size // 2 + 32, size), BF16),
            pltpu.VMEM((halves, size // 2 + 32, size), BF16),
            pltpu.VMEM((n_chan, 2, tall, size), F32),
            pltpu.VMEM((2, tall, size), F32),
            pltpu.VMEM((2, tall, size), F32),
            pltpu.VMEM((n_chan, size, size), BF16),
            pltpu.VMEM((n_chan, size, size), BF16),
            sem((6 + fpb * nnz,)),
            sem((nfx,)),
            sem((nfx,)),
            sem((halves, nfx)),
            sem((halves, nfx)),
            sem((halves, nfx)),
            sem((halves, nfx)),
            sem((halves, 8)),
            sem((halves, 8)),
            sem((n_chan,)),
            sem((n_chan,)),
        ],
        compiler_params=pltpu.CompilerParams(
            collective_id=0, has_side_effects=True, vmem_limit_bytes=24 * 2**20
        ),
    )(
        pinned(sky),
        pinned(vis[0, 0]),
        pinned(weights[0, 0]),
        pinned(tiles[0, 0].transpose(1, 2, 0)),
        pinned(lists.reshape(-1)),
        count.reshape(-1),
        pinned(threshold),
        pinned(jnp.asarray(tables(size))),
    )
    square = pltpu.VMEM((4 * n_chan * n_chan, size), F32)
    return pl.pallas_call(
        last_kernel,
        out_shape=jax.ShapeDtypeStruct((n_chan, size, size), F32),
        in_specs=[vmem, vmem, smem],
        out_specs=vmem,
        scratch_shapes=[square, square, square],
        compiler_params=pltpu.CompilerParams(vmem_limit_bytes=8 * 2**20),
    )(shr, other, weight.reshape(1))


def solution(mesh):
    in_specs = (
        P("blk", "fy", "fx"),
        P("fy", "fx", "blk", None, None),
        P("fy", "fx", None, None, None, None, None),
        P("fy", "fx", None, None, None),
        P("fy", "fx", None),
        P("fy", "fx"),
        P(None, "blk"),
        P(),
    )

    def step(*args):
        fpb, vt, nnz = args[3].shape[2:]
        sizes = (mesh.shape["fx"], mesh.shape["fy"], mesh.shape["blk"], fpb, vt, nnz, 2)
        return body(sizes, *args)

    return jax.shard_map(
        step, mesh=mesh, in_specs=in_specs, out_specs=P("blk", "fy", "fx"), check_vma=False
    )
```

```python
import functools
import math

import jax
import jax.numpy as jnp
import ml_dtypes
import numpy as np
from jax import lax
from jax.experimental import pallas as pl
from jax.experimental.pallas import tpu as pltpu
from jax.sharding import PartitionSpec as P

MESH = pl.DeviceIdType.MESH
F32 = jnp.float32
BF16 = jnp.bfloat16
STEP = 2.0


def tables(length):
    positions = np.arange(length)
    angles = (positions[:, None] * positions[None, :] % length) * (2.0 * math.pi / length)
    cosine = (np.cos(angles) / math.sqrt(length)).astype(np.float32)
    sinus = (np.sin(angles) / math.sqrt(length)).astype(np.float32)
    whole = np.concatenate(
        [np.concatenate([cosine, -sinus], axis=1), np.concatenate([sinus, cosine], axis=1)], axis=0
    )
    high = whole.astype(ml_dtypes.bfloat16)
    low = (whole - high.astype(np.float32)).astype(ml_dtypes.bfloat16)
    return np.stack([high, low])


def smoothers(size, levels, margin):
    reach = np.arange(-2 * margin, size + 2 * margin)
    apart = np.abs(reach[:, None] - reach[None, :])
    out = np.zeros((3, 2 * size, levels * size), np.float64)
    for variant in range(3):
        alive = np.ones(len(reach))
        if variant == 0:
            alive[reach < 0] = 0
        if variant == 2:
            alive[reach >= size] = 0
        whole = np.diag(alive)
        for level in range(levels):
            one = 2.0 * (apart == 0) + 1.0 * (apart == 2**level)
            whole = alive[:, None] * (one @ whole)
            taps = (whole / 16.0 ** (level + 1))[2 * margin : 2 * margin + size].T
            span = slice(level * size, (level + 1) * size)
            out[variant, :size, span] = taps[2 * margin : 2 * margin + size]
            out[variant, size : size + margin, span] = taps[2 * margin + size : 3 * margin + size]
            out[variant, 2 * size - margin :, span] = taps[margin : 2 * margin]
    return out.astype(ml_dtypes.bfloat16)


def dot(a, b):
    return jnp.dot(a, b, preferred_element_type=F32)


def dot_nt(a, b):
    return lax.dot_general(a, b, (((1,), (1,)), ((), ())), preferred_element_type=F32)


def dot_tn(a, b):
    return lax.dot_general(a, b, (((0,), (0,)), ((), ())), preferred_element_type=F32)


def split(values):
    high = values.astype(BF16)
    return high, (values - high.astype(F32)).astype(BF16)


def dot3(a, b):
    return dot(a[0], b[0]) + (dot(a[0], b[1]) + dot(a[1], b[0]))


def pinned(array):
    return pltpu.with_memory_space_constraint(array, pltpu.HBM)


def kernel(
    sizes,
    sky_hbm,
    vis_hbm,
    w_hbm,
    tiles_hbm,
    list_hbm,
    count_s,
    thr_hbm,
    tab_hbm,
    smooth_hbm,
    shr,
    other,
    tiles_s,
    list_s,
    sky_v,
    vis_v,
    wv,
    tab,
    smooth,
    idx_send,
    idx_recv,
    spec,
    row_send,
    row_recv0,
    row_recv1,
    con_buf,
    con_send,
    con_recv,
    inv_s,
    slot_s,
    place_mat,
    st_bf,
    mate_bf,
    edge_send,
    top_recv,
    bot_recv,
    vl,
    vr,
    hi_buf,
    ybuf,
    zbuf,
    thr_v,
    thr_mate,
    bounds,
    local_sem,
    idx_ssem,
    idx_rsem,
    row_ssem,
    row_rsem,
    con_ssem,
    con_rsem,
    halo_ssem,
    halo_rsem,
    thr_sem,
):
    nfx, nfy, nblk, fpb, vt, nnz, halves = sizes
    n_chan, size, _ = sky_v.shape
    per = n_chan // halves
    row_recv = (row_recv0, row_recv1)
    slots = vt * nnz
    lanes = nfx * 2 * slots
    fy, fx, blk = lax.axis_index("fy"), lax.axis_index("fx"), lax.axis_index("blk")

    def along_fx(d):
        return (fy, lax.rem(fx + d, nfx), blk)

    up, down = lax.rem(fy + nfy - 1, nfy), lax.rem(fy + 1, nfy)
    left, right = lax.rem(fx + nfx - 1, nfx), lax.rem(fx + 1, nfx)
    mate = (fy, fx, 1 - blk)
    order = sorted(range(1, nfx), key=lambda d: -min(d, nfx - d))
    far = [d for d in order if min(d, nfx - d) > nfx // 4]
    near = [d for d in order if d not in far]
    slot = {d: k for k, d in enumerate([0] + near + far)}

    loads = []

    def load(src, dst):
        copy = pltpu.make_async_copy(src, dst, local_sem.at[len(loads)])
        copy.start()
        loads.append(copy)
        return copy

    barrier = pltpu.get_barrier_semaphore()
    others = [along_fx(d) for d in order]
    around = [(up, fx), (down, fx), (fy, left), (fy, right)]
    around += [(r, c) for r in (up, down) for c in (left, right)]
    others += [(up, fx, blk), (down, fx, blk), mate]
    others += [(r, c, blk) for r in (up, down) for c in (left, right)]
    others += [(r, c, 1 - blk) for r, c in around]
    for device in others:
        pl.semaphore_signal(barrier, inc=1, device_id=device, device_id_type=MESH)

    small_loads = [
        load(tiles_hbm, tiles_s),
        load(list_hbm, list_s),
    ]
    thr_load = load(thr_hbm, thr_v)
    tab_load = load(tab_hbm, tab)
    sky_load = load(sky_hbm, sky_v)
    vis_load = load(vis_hbm, vis_v)
    w_loads = [
        load(w_hbm.at[f, :, n], wv.at[f // 2, n, :, :, pl.ds((f % 2) * size, size)])
        for f in range(fpb)
        for n in range(nnz)
    ]
    edge_kind = (fx + nfx - 2) // (nfx - 1) + fx // (nfx - 1)
    smooth_load = load(smooth_hbm.at[edge_kind], smooth)

    for copy in small_loads:
        copy.wait()
    lane = lax.broadcasted_iota(jnp.int32, (1, lanes), 1)
    lane_a, lane_n = lane % vt, (lane // vt) % nnz
    lane_p, lane_j = (lane // slots) % 2, lane // (2 * slots)
    wanted = []
    for f in range(fpb):
        row = jnp.zeros((1, lanes), jnp.int32)
        for a in range(vt):
            for n in range(nnz):
                here = (lane_a == a) & (lane_n == n)
                row = jnp.where(here, tiles_s[a, n, f], row)
        wanted.append(row + lane_p * size + 1)
    where_f = [0] * fpb
    for d in range(nfx):
        owner = lax.rem(fx + d, nfx)
        request = jnp.zeros((1, lanes), jnp.int32)
        place = fpb
        for f in range(fpb):
            hit = list_s[f] == owner
            request = jnp.where(hit, wanted[f], request)
            place = jnp.where(hit, f, place)
            where_f[f] = jnp.where(hit, slot[d], where_f[f])
        idx_send[slot[d]] = jnp.where(lane_j == slot[d], request, 0)
        inv_s[slot[d]] = place
    for f in range(fpb):
        slot_s[f] = where_f[f]
    idx_recv[0] = idx_send[0]

    pl.semaphore_wait(barrier, len(others))

    def exchange(send, recv, ssem, rsem, sign=1, peers=order):
        copies = []
        for d in peers:
            copy = pltpu.make_async_remote_copy(
                src_ref=send.at[slot[d]],
                dst_ref=recv.at[slot[d]],
                send_sem=ssem.at[d],
                recv_sem=rsem.at[d],
                device_id=along_fx(d if sign > 0 else nfx - d),
                device_id_type=MESH,
            )
            copy.start()
            copies.append(copy)
        return copies

    idx_copies = exchange(idx_send, idx_recv, idx_ssem, idx_rsem)
    thr_load.wait()
    thr_copy = pltpu.make_async_remote_copy(
        src_ref=thr_v,
        dst_ref=thr_mate,
        send_sem=thr_sem.at[0],
        recv_sem=thr_sem.at[1],
        device_id=mate,
        device_id_type=MESH,
    )
    thr_copy.start()

    tab_load.wait()
    sky_load.wait()
    high = tab[0]
    left_table = jnp.concatenate([high[:size, :size], high[:size, size:]], axis=0)
    for c in range(n_chan):
        half = dot(left_table, sky_v[c]).astype(BF16)
        half = jnp.concatenate([half[:size], half[size:]], axis=1)
        full = dot(half, high).astype(BF16)
        spec[:size, c * size : (c + 1) * size] = full[:, :size]
        spec[size:, c * size : (c + 1) * size] = full[:, size:]

    row_ids = lax.broadcasted_iota(jnp.int32, (2 * size, lanes), 0) + 1
    group = 2 * slots
    row_copies = [[] for _ in range(halves)]
    for k, peers in enumerate((near, far)):
        for copy, d in zip(idx_copies, order):
            if d in peers:
                copy.wait_recv()
        first, count = (0, 1 + len(near)) if k == 0 else (1 + len(near), len(far))
        span_k = slice(first * group, (first + count) * group)
        target = idx_recv[first, :, span_k]
        for e in range(first + 1, first + count):
            target = target + idx_recv[e, :, span_k]
        mat = jnp.where(row_ids[:, : count * group] == target, 1.0, 0.0).astype(BF16)
        place_mat[:, span_k] = mat
        for h in range(halves):
            span = slice(h * per * size, (h + 1) * per * size)
            picked = dot_tn(mat, spec[:, span]).reshape(count, 2, 1, slots, per * size)
            picked = jnp.concatenate(
                [picked[..., c * size : (c + 1) * size] for c in range(per)], axis=2
            )
            row_send[h, first : first + count] = picked.reshape(count, per * group, size).astype(BF16)
            if k == 0:
                row_recv[h][0] = row_send[h, 0]
            row_copies[h] += exchange(
                row_send.at[h], row_recv[h], row_ssem.at[h], row_rsem.at[h], -1, peers
            )

    rows_all = per * group
    n_vis = vt * size
    vis_load.wait()
    row_id = lax.broadcasted_iota(jnp.int32, (rows_all, n_vis), 0)
    vis_id = lax.broadcasted_iota(jnp.int32, (rows_all, n_vis), 1)
    live = (vis_id < count_s[0]) & (row_id % vt == vis_id // size)
    first_slot = (row_id // vt) % nnz == 0
    first_out = (lax.broadcasted_iota(jnp.int32, (rows_all, 2 * size), 0) // vt) % nnz == 0
    for h in range(halves):
        con_buf[h, fpb] = jnp.zeros((rows_all, size), BF16)
    for copy in w_loads:
        copy.wait()

    con_copies = []
    for h in range(halves):
        for copy in row_copies[h]:
            copy.wait_recv()
        measured = []
        for p in range(2):
            for c in range(per):
                both = vis_v[h * per + c].astype(F32)
                measured.append(jnp.broadcast_to(both[p : p + 1], (slots, n_vis)))
        measured = jnp.concatenate(measured, axis=0)
        sums = [None, None]
        for q in range(fpb // 2):
            x = jnp.concatenate(
                [row_recv[h][slot_s[2 * q]], row_recv[h][slot_s[2 * q + 1]]], axis=1
            )
            for n in range(nnz):
                term = dot_nt(x, wv[q, n].reshape(n_vis, 2 * size))
                sums[n] = term if sums[n] is None else sums[n] + term
        mixed = jnp.where(first_slot, sums[0], sums[1])
        later = pltpu.roll(mixed, rows_all - vt, 0)
        earlier = pltpu.roll(mixed, vt, 0)
        predicted = mixed + jnp.where(first_slot, later, earlier)
        residual = jnp.where(live, predicted - measured, 0.0).astype(BF16)
        for q in range(fpb // 2):
            terms = [dot(residual, wv[q, n].reshape(n_vis, 2 * size)) for n in range(nnz)]
            out = jnp.where(first_out, terms[0], terms[1]).astype(BF16)
            con_buf[h, 2 * q] = out[:, :size]
            con_buf[h, 2 * q + 1] = out[:, size:]
        for k in range(nfx):
            con_send[h, k] = con_buf[h, inv_s[k]]
        con_recv[h, 0] = con_send[h, 0]
        con_copies.append(
            exchange(con_send.at[h], con_recv.at[h], con_ssem.at[h], con_rsem.at[h])
        )

    def flipped(table):
        return jnp.concatenate(
            [
                jnp.concatenate([table[:size, :size], table[size:, :size]], axis=1),
                jnp.concatenate([table[:size, size:], table[size:, size:]], axis=1),
            ],
            axis=0,
        )

    right_back = (flipped(tab[0]), flipped(tab[1]))
    left_back = tuple(dot(tab[k, :size, :], place_mat[...]).astype(BF16) for k in range(2))
    lane_id = lax.broadcasted_iota(jnp.int32, (1, size), 1)
    quarter = size // 4
    halo_copies = []
    for h in range(halves):
        for copy in con_copies[h]:
            copy.wait_recv()
        own_rows = per * slots
        incoming = jnp.concatenate(
            [
                con_recv[h, :, p * own_rows : (p + 1) * own_rows, :].reshape(nfx * own_rows, size)
                for p in range(2)
            ],
            axis=1,
        )
        half = dot(incoming, right_back[0]) + dot(incoming, right_back[1])
        half = half.reshape(nfx, per, slots, 2 * size)
        half = jnp.concatenate(
            [
                jnp.concatenate(
                    [half[:, c : c + 1, :, p * size : (p + 1) * size] for p in range(2)], axis=1
                ).reshape(nfx * group, size)
                for c in range(per)
            ],
            axis=1,
        )
        grad = dot3(left_back, split(half))
        edges = [jnp.zeros((quarter, size), F32) for _ in range(2)]
        for c in range(per):
            stepped = sky_v[h * per + c].astype(F32) - STEP * grad[:, c * size : (c + 1) * size]
            shr[h * per + c] = stepped
            high = stepped.astype(BF16)
            st_bf[h, c] = high
            hi_buf[h, c, 16 : 16 + size, :size] = high
            for fold in range(4):
                at = 32 * fold + 16 * c
                part = stepped[fold * quarter : (fold + 1) * quarter]
                hit = (lane_id >= at) & (lane_id < at + 16)
                for e, turn in enumerate((at, (at + 16) % size)):
                    moved = pltpu.roll(part, turn, 1) if turn else part
                    edges[e] = jnp.where(hit, moved, edges[e])
        for e in range(2):
            edge_send[h, e] = edges[e].astype(BF16)

        first, last = pl.ds(0, 16), pl.ds(quarter - 16, 16)
        main, low = pl.ds(16, quarter), pl.ds(16 + quarter, 16)
        copies = []

        def send(src, dst, device, who, k):
            copy = pltpu.make_async_remote_copy(
                src_ref=src,
                dst_ref=dst,
                send_sem=halo_ssem.at[h, who, k],
                recv_sem=halo_rsem.at[h, who, k],
                device_id=device,
                device_id_type=MESH,
            )
            copy.start()
            copies.append(copy)

        send(st_bf.at[h], mate_bf.at[h], mate, 1, 8)
        for who, where in ((0, blk), (1, 1 - blk)):
            top, bottom = top_recv.at[h, who], bot_recv.at[h, who]
            fl, fr = vl.at[h, who], vr.at[h, who]
            halo = [
                (edge_send.at[h, 0, first], fr.at[low], (up, left, where)),
                (edge_send.at[h, 1, first], fl.at[low], (up, right, where)),
                (edge_send.at[h, 0, last], fr.at[first], (down, left, where)),
                (edge_send.at[h, 1, last], fl.at[first], (down, right, where)),
                (edge_send.at[h, 0], fr.at[main], (fy, left, where)),
                (edge_send.at[h, 1], fl.at[main], (fy, right, where)),
                (st_bf.at[h, :, pl.ds(0, 16), :], bottom, (up, fx, where)),
                (st_bf.at[h, :, pl.ds(size - 16, 16), :], top, (down, fx, where)),
            ]
            for k, (src, dst, device) in enumerate(halo):
                send(src, dst, device, who, k)
        halo_copies.append(copies)

    tall = size + 32
    streams = 2 * per
    in_top, in_bottom = fy > 0, fy < nfy - 1
    row_tall = lax.broadcasted_iota(jnp.int32, (tall, 1), 0)
    rows_live = ((row_tall >= 16) | in_top) & ((row_tall < 16 + size) | in_bottom)
    zeros8 = jnp.zeros((8, size), F32)
    levels = thr_v.shape[0]
    thr_copy.wait_recv()
    for who, part in enumerate((thr_v, thr_mate)):
        for c in range(n_chan):
            for level in range(levels):
                at = (who * n_chan + c) * levels + level
                value = part[level : level + 1, c : c + 1]
                bounds[at : at + 1, :] = jnp.broadcast_to(value, (1, size))
    for buf in (ybuf, zbuf):
        for q in range(streams):
            for level in range(1, levels):
                buf[q, level, 0:8, :] = zeros8
                buf[q, level, 8 + tall : 16 + tall, :] = zeros8
    smooth_load.wait()
    for copies in [idx_copies, [thr_copy]] + row_copies + con_copies:
        for copy in copies:
            copy.wait_send()
    pieces = [(0, 0, 16, 3), (16 + size, 16 + quarter, 16, 0)]
    pieces += [(16 + k * quarter, 16, quarter, k) for k in range(4)]

    def summed(ref, at, count, s):
        x = ref[at : at + count, :]
        return (ref[at - s : at - s + count, :] + x) + (ref[at + s : at + s + count, :] + x)

    for h in range(halves):
        for copy in halo_copies[h]:
            copy.wait_recv()
        for who in range(2):
            from_left = vl[h, who].astype(F32)
            from_right = vr[h, who].astype(F32)
            for c in range(per):
                q = who * per + c
                if who == 1:
                    hi_buf[h, q, 16 : 16 + size, :size] = mate_bf[h, c]
                hi_buf[h, q, 0:16, :size] = jnp.where(
                    in_top, top_recv[h, who, c].astype(F32), 0.0
                ).astype(BF16)
                hi_buf[h, q, 16 + size :, :size] = jnp.where(
                    in_bottom, bot_recv[h, who, c].astype(F32), 0.0
                ).astype(BF16)
                for to, start, count, fold in pieces:
                    at = 32 * fold + 16 * c
                    r = from_right[start : start + count]
                    r = pltpu.roll(r, size - at, 1) if at else r
                    l = pltpu.roll(from_left[start : start + count], (2 * size - 16 - at) % size, 1)
                    side = jnp.where(lane_id < 64, r, l)
                    if to in (0, 16 + size):
                        side = jnp.where(rows_live[to : to + count], side, 0.0)
                    hi_buf[h, q, to : to + count, size:] = side.astype(BF16)
        for t in range(levels // 2):
            span = slice(2 * t * size, 2 * (t + 1) * size)
            result = dot(hi_buf[h].reshape(streams * tall, 2 * size), smooth[:, span])
            for q in range(streams):
                for e in range(2):
                    ybuf[q, 2 * t + e, 8 : 8 + tall, :] = result[
                        q * tall : (q + 1) * tall, e * size : (e + 1) * size
                    ]
        for q in range(streams):
            who, c = q // per, h * per + q % per
            sources = [ybuf.at[q, 0]]
            for level in range(1, levels):
                source, dest = ybuf.at[q, level], zbuf.at[q, level]
                reach = 2 ** (level + 1) - 2
                for step in range(level):
                    s = 2**step
                    reach -= s if step else 0
                    low, top = (24 - reach) // 8 * 8, (24 + size + reach + 7) // 8 * 8
                    for at, stop in ((low, 24), (24 + size, top)):
                        part = summed(source, at, stop - at, s)
                        dest[at:stop, :] = jnp.where(rows_live[at - 8 : stop - 8], part, 0.0)
                    for at in range(24, 24 + size, 32):
                        dest[at : at + 32, :] = summed(source, at, 32, s)
                    source, dest = dest, source
                sources.append(source)
            for at in range(0, size, 16):
                rows = slice(at, at + 16)
                value = shr[c, rows, :] if who == 0 else mate_bf[h, q % per, rows, :].astype(F32)
                coarse = value
                for level in range(levels):
                    at_bound = (who * n_chan + c) * levels + level
                    bound = bounds[at_bound : at_bound + 1, :]
                    finer = summed(sources[level], 24 + at, 16, 2**level)
                    value = value - jnp.minimum(jnp.maximum(coarse - finer, -bound), bound)
                    coarse = finer
                if who == 0:
                    shr[c, rows, :] = value
                else:
                    other[c, rows, :] = value

    for copies in halo_copies:
        for copy in copies:
            copy.wait_send()


def last_kernel(shr, other, mu_s, out_ref, gpart, gtot, xs):
    n_chan, size, _ = shr.shape
    total = 2 * n_chan
    chunk = 16
    pairs = [(a, b) for a in range(total) for b in range(a, total)]

    def step(i, sums):
        rows = pl.ds(pl.multiple_of(i * chunk, chunk), chunk)
        vals = [shr[c, rows, :] for c in range(n_chan)]
        vals += [other[c, rows, :].astype(F32) for c in range(n_chan)]
        news = []
        for k, (a, b) in enumerate(pairs):
            prod = vals[a] * vals[b]
            news.append(sums[k] + (prod[:8] + prod[8:]))
        return tuple(news)

    sums = lax.fori_loop(
        0, size // chunk, step, tuple(jnp.zeros((8, size), F32) for _ in pairs)
    )
    for (a, b), value in zip(pairs, sums):
        value = jnp.sum(value, axis=0, keepdims=True)
        gpart[a * total + b : a * total + b + 1, :] = value
        if a != b:
            gpart[b * total + a : b * total + a + 1, :] = value
    gtot[...] = jnp.broadcast_to(jnp.sum(gpart[...], axis=1, keepdims=True), gtot.shape)

    mu = mu_s[0] * float(size * size)
    mat = {}
    for a, b in pairs:
        value = jnp.broadcast_to(gtot[a * total + b : a * total + b + 1, :], (total, size))
        mat[a, b] = value + mu if a == b else value
    rhs = [gtot[c * total : (c + 1) * total, :] for c in range(total)]
    inverse = [None] * total
    for k in range(total):
        inverse[k] = 1.0 / mat[k, k]
        for i in range(k + 1, total):
            factor = mat[k, i] * inverse[k]
            for j in range(i, total):
                mat[i, j] = mat[i, j] - factor * mat[k, j]
            rhs[i] = rhs[i] - factor * rhs[k]
    solved = [None] * total
    for k in range(total - 1, -1, -1):
        value = rhs[k]
        for i in range(k + 1, total):
            value = value - mat[k, i] * solved[i]
        solved[k] = value * inverse[k]
        xs[k * total : (k + 1) * total, :] = solved[k]

    coeffs = [
        [jnp.broadcast_to(xs[c * total + d : c * total + d + 1, :], (8, size)) for c in range(total)]
        for d in range(n_chan)
    ]

    def finish(i, carry):
        rows = pl.ds(pl.multiple_of(i * chunk, chunk), chunk)
        vals = [shr[c, rows, :] for c in range(n_chan)]
        vals += [other[c, rows, :].astype(F32) for c in range(n_chan)]
        for d in range(n_chan):
            for h in range(2):
                value = coeffs[d][0] * vals[0][h * 8 : h * 8 + 8]
                for c in range(1, total):
                    value = value + coeffs[d][c] * vals[c][h * 8 : h * 8 + 8]
                out_ref[d, pl.ds(pl.multiple_of(i * chunk + h * 8, 8), 8), :] = value
        return carry

    lax.fori_loop(0, size // chunk, finish, 0)


def body(sizes, sky, vis, weights, tiles, lists, count, threshold, weight):
    nfx, nfy, nblk, fpb, vt, nnz, halves = sizes
    n_chan, size, _ = sky.shape
    per = n_chan // halves
    rows = per * 2 * vt * nnz
    lanes = nfx * 2 * vt * nnz
    hbm = pl.BlockSpec(memory_space=pltpu.HBM)
    smem = pl.BlockSpec(memory_space=pltpu.SMEM)
    vmem = pl.BlockSpec(memory_space=pltpu.VMEM)
    tall = size + 48
    levels = threshold.shape[0]
    sem = pltpu.SemaphoreType.DMA
    shr, other = pl.pallas_call(
        functools.partial(kernel, sizes),
        out_shape=[
            jax.ShapeDtypeStruct((n_chan, size, size), F32),
            jax.ShapeDtypeStruct((n_chan, size, size), F32),
        ],
        in_specs=[hbm] * 5 + [smem, hbm, hbm, hbm],
        out_specs=[vmem, vmem],
        scratch_shapes=[
            pltpu.SMEM((vt, nnz, fpb), jnp.int32),
            pltpu.SMEM((fpb,), jnp.int32),
            pltpu.VMEM((n_chan, size, size), BF16),
            pltpu.VMEM((n_chan, 2, vt * size), BF16),
            pltpu.VMEM((fpb // 2, nnz, vt, size, 2 * size), BF16),
            pltpu.VMEM((2, 2 * size, 2 * size), BF16),
            pltpu.VMEM((2 * size, levels * size), BF16),
            pltpu.VMEM((nfx, 1, lanes), jnp.int32),
            pltpu.VMEM((nfx, 1, lanes), jnp.int32),
            pltpu.VMEM((2 * size, n_chan * size), BF16),
            pltpu.VMEM((halves, nfx, rows, size), BF16),
            pltpu.VMEM((nfx, rows, size), BF16),
            pltpu.VMEM((nfx, rows, size), BF16),
            pltpu.VMEM((halves, fpb + 1, rows, size), BF16),
            pltpu.VMEM((halves, nfx, rows, size), BF16),
            pltpu.VMEM((halves, nfx, rows, size), BF16),
            pltpu.SMEM((nfx,), jnp.int32),
            pltpu.SMEM((fpb,), jnp.int32),
            pltpu.VMEM((2 * size, lanes), BF16),
            pltpu.VMEM((halves, per, size, size), BF16),
            pltpu.VMEM((halves, per, size, size), BF16),
            pltpu.VMEM((halves, 2, size // 4, size), BF16),
            pltpu.VMEM((halves, 2, per, 16, size), BF16),
            pltpu.VMEM((halves, 2, per, 16, size), BF16),
            pltpu.VMEM((halves, 2, size // 4 + 32, size), BF16),
            pltpu.VMEM((halves, 2, size // 4 + 32, size), BF16),
            pltpu.VMEM((halves, 2 * per, size + 32, 2 * size), BF16),
            pltpu.VMEM((2 * per, levels, tall, size), F32),
            pltpu.VMEM((2 * per, levels, tall, size), F32),
            pltpu.VMEM(threshold.shape, F32),
            pltpu.VMEM(threshold.shape, F32),
            pltpu.VMEM((2 * n_chan * levels, size), F32),
            sem((7 + fpb * nnz,)),
            sem((nfx,)),
            sem((nfx,)),
            sem((halves, nfx)),
            sem((halves, nfx)),
            sem((halves, nfx)),
            sem((halves, nfx)),
            sem((halves, 2, 9)),
            sem((halves, 2, 9)),
            sem((2,)),
        ],
        compiler_params=pltpu.CompilerParams(
            collective_id=0, has_side_effects=True, vmem_limit_bytes=24 * 2**20
        ),
    )(
        pinned(sky),
        pinned(vis[0, 0]),
        pinned(weights[0, 0]),
        pinned(tiles[0, 0].transpose(1, 2, 0)),
        pinned(lists.reshape(-1)),
        count.reshape(-1),
        pinned(threshold),
        pinned(jnp.asarray(tables(size))),
        pinned(jnp.asarray(smoothers(size, levels, 16))),
    )
    square = pltpu.VMEM((4 * n_chan * n_chan, size), F32)
    return pl.pallas_call(
        last_kernel,
        out_shape=jax.ShapeDtypeStruct((n_chan, size, size), F32),
        in_specs=[vmem, vmem, smem],
        out_specs=vmem,
        scratch_shapes=[square, square, square],
        compiler_params=pltpu.CompilerParams(vmem_limit_bytes=8 * 2**20),
    )(shr, other, weight.reshape(1))


def solution(mesh):
    in_specs = (
        P("blk", "fy", "fx"),
        P("fy", "fx", "blk", None, None),
        P("fy", "fx", None, None, None, None, None),
        P("fy", "fx", None, None, None),
        P("fy", "fx", None),
        P("fy", "fx"),
        P(None, "blk"),
        P(),
    )

    def step(*args):
        fpb, vt, nnz = args[3].shape[2:]
        sizes = (mesh.shape["fx"], mesh.shape["fy"], mesh.shape["blk"], fpb, vt, nnz, 2)
        return body(sizes, *args)

    return jax.shard_map(
        step, mesh=mesh, in_specs=in_specs, out_specs=P("blk", "fy", "fx"), check_vma=False
    )
```

```python
import functools
import math

import jax
import jax.numpy as jnp
import ml_dtypes
import numpy as np
from jax import lax
from jax.experimental import pallas as pl
from jax.experimental.pallas import tpu as pltpu
from jax.sharding import PartitionSpec as P

MESH = pl.DeviceIdType.MESH
F32 = jnp.float32
BF16 = jnp.bfloat16
STEP = 2.0


def tables(length):
    positions = np.arange(length)
    angles = (positions[:, None] * positions[None, :] % length) * (2.0 * math.pi / length)
    cosine = (np.cos(angles) / math.sqrt(length)).astype(np.float32)
    sinus = (np.sin(angles) / math.sqrt(length)).astype(np.float32)
    whole = np.concatenate(
        [np.concatenate([cosine, -sinus], axis=1), np.concatenate([sinus, cosine], axis=1)], axis=0
    )
    high = whole.astype(ml_dtypes.bfloat16)
    low = (whole - high.astype(np.float32)).astype(ml_dtypes.bfloat16)
    return np.stack([high, low])


def smoothers(size, levels, margin):
    reach = np.arange(-2 * margin, size + 2 * margin)
    apart = np.abs(reach[:, None] - reach[None, :])
    out = np.zeros((3, 2 * size, levels * size), np.float64)
    for variant in range(3):
        alive = np.ones(len(reach))
        if variant == 0:
            alive[reach < 0] = 0
        if variant == 2:
            alive[reach >= size] = 0
        whole = np.diag(alive)
        for level in range(levels):
            one = 2.0 * (apart == 0) + 1.0 * (apart == 2**level)
            whole = alive[:, None] * (one @ whole)
            taps = (whole / 16.0 ** (level + 1))[2 * margin : 2 * margin + size].T
            span = slice(level * size, (level + 1) * size)
            out[variant, :size, span] = taps[2 * margin : 2 * margin + size]
            out[variant, size : size + margin, span] = taps[2 * margin + size : 3 * margin + size]
            out[variant, 2 * size - margin :, span] = taps[margin : 2 * margin]
    return out.astype(ml_dtypes.bfloat16)


def dot(a, b):
    return jnp.dot(a, b, preferred_element_type=F32)


def dot_nt(a, b):
    return lax.dot_general(a, b, (((1,), (1,)), ((), ())), preferred_element_type=F32)


def dot_tn(a, b):
    return lax.dot_general(a, b, (((0,), (0,)), ((), ())), preferred_element_type=F32)


def split(values):
    high = values.astype(BF16)
    return high, (values - high.astype(F32)).astype(BF16)


def dot3(a, b):
    return dot(a[0], b[0]) + (dot(a[0], b[1]) + dot(a[1], b[0]))


def pinned(array):
    return pltpu.with_memory_space_constraint(array, pltpu.HBM)


def kernel(
    sizes,
    sky_hbm,
    vis_hbm,
    w_hbm,
    tiles_hbm,
    list_hbm,
    count_s,
    thr_hbm,
    tab_hbm,
    smooth_hbm,
    shr,
    other,
    tiles_s,
    list_s,
    sky_v,
    vis_v,
    wv,
    tab,
    smooth,
    idx_send,
    idx_recv,
    spec,
    row_send,
    row_recv0,
    row_recv1,
    con_buf,
    con_send,
    con_recv,
    inv_s,
    slot_s,
    place_mat,
    st_bf,
    edge_send,
    halo_recv,
    hi_buf,
    ybuf,
    zbuf,
    thr_v,
    thr_mate,
    bounds,
    local_sem,
    idx_ssem,
    idx_rsem,
    row_ssem,
    row_rsem,
    con_ssem,
    con_rsem,
    halo_ssem,
    halo_rsem,
    thr_sem,
):
    nfx, nfy, nblk, fpb, vt, nnz, halves = sizes
    n_chan, size, _ = sky_v.shape
    per = n_chan // halves
    row_recv = (row_recv0, row_recv1)
    slots = vt * nnz
    lanes = nfx * 2 * slots
    fy, fx, blk = lax.axis_index("fy"), lax.axis_index("fx"), lax.axis_index("blk")

    def along_fx(d):
        return (fy, lax.rem(fx + d, nfx), blk)

    up, down = lax.rem(fy + nfy - 1, nfy), lax.rem(fy + 1, nfy)
    left, right = lax.rem(fx + nfx - 1, nfx), lax.rem(fx + 1, nfx)
    mate = (fy, fx, 1 - blk)
    order = sorted(range(1, nfx), key=lambda d: -min(d, nfx - d))
    far = [d for d in order if min(d, nfx - d) > nfx // 4]
    near = [d for d in order if d not in far]
    slot = {d: k for k, d in enumerate([0] + near + far)}

    loads = []

    def arrived(buffer, semaphore):
        pltpu.make_async_copy(buffer, buffer, semaphore).wait()

    def load(src, dst):
        copy = pltpu.make_async_copy(src, dst, local_sem.at[len(loads)])
        copy.start()
        loads.append(copy)
        return copy

    barrier = pltpu.get_barrier_semaphore()
    others = [along_fx(d) for d in order]
    around = [(up, fx), (down, fx), (fy, left), (fy, right)]
    around += [(r, c) for r in (up, down) for c in (left, right)]
    others += [(up, fx, blk), (down, fx, blk), mate]
    others += [(r, c, blk) for r in (up, down) for c in (left, right)]
    others += [(r, c, 1 - blk) for r, c in around]
    for device in others:
        pl.semaphore_signal(barrier, inc=1, device_id=device, device_id_type=MESH)

    small_loads = [
        load(tiles_hbm, tiles_s),
        load(list_hbm, list_s),
    ]
    thr_load = load(thr_hbm, thr_v)
    tab_load = load(tab_hbm, tab)
    sky_load = load(sky_hbm, sky_v)
    vis_load = load(vis_hbm, vis_v)
    for f in range(fpb):
        for n in range(nnz):
            pltpu.make_async_copy(
                w_hbm.at[f, :, n],
                wv.at[f // 2, n, :, :, pl.ds((f % 2) * size, size)],
                local_sem.at[local_sem.shape[0] - 1],
            ).start()
    edge_kind = (fx + nfx - 2) // (nfx - 1) + fx // (nfx - 1)
    smooth_load = load(smooth_hbm.at[edge_kind], smooth)

    for copy in small_loads:
        copy.wait()
    lane = lax.broadcasted_iota(jnp.int32, (1, lanes), 1)
    lane_a, lane_n = lane % vt, (lane // vt) % nnz
    lane_p, lane_j = (lane // slots) % 2, lane // (2 * slots)
    wanted = []
    for f in range(fpb):
        row = jnp.zeros((1, lanes), jnp.int32)
        for a in range(vt):
            for n in range(nnz):
                here = (lane_a == a) & (lane_n == n)
                row = jnp.where(here, tiles_s[a, n, f], row)
        wanted.append(row + lane_p * size + 1)
    where_f = [0] * fpb
    for d in range(nfx):
        owner = lax.rem(fx + d, nfx)
        request = jnp.zeros((1, lanes), jnp.int32)
        place = fpb
        for f in range(fpb):
            hit = list_s[f] == owner
            request = jnp.where(hit, wanted[f], request)
            place = jnp.where(hit, f, place)
            where_f[f] = jnp.where(hit, slot[d], where_f[f])
        idx_send[slot[d]] = jnp.where(lane_j == slot[d], request, 0)
        inv_s[slot[d]] = place
    for f in range(fpb):
        slot_s[f] = where_f[f]
    idx_recv[0] = idx_send[0]

    pl.semaphore_wait(barrier, len(others))

    def exchange(send, recv, ssem, rsem, sign=1, peers=order):
        for d in peers:
            pltpu.make_async_remote_copy(
                src_ref=send.at[slot[d]],
                dst_ref=recv.at[slot[d]],
                send_sem=ssem,
                recv_sem=rsem if peers is order or sign < 0 else rsem.at[int(d in far)],
                device_id=along_fx(d if sign > 0 else nfx - d),
                device_id_type=MESH,
            ).start()

    exchange(idx_send, idx_recv, idx_ssem.at[0], idx_rsem, 1, far)
    exchange(idx_send, idx_recv, idx_ssem.at[0], idx_rsem, 1, near)
    thr_load.wait()
    thr_copy = pltpu.make_async_remote_copy(
        src_ref=thr_v,
        dst_ref=thr_mate,
        send_sem=thr_sem.at[0],
        recv_sem=thr_sem.at[1],
        device_id=mate,
        device_id_type=MESH,
    )
    thr_copy.start()

    tab_load.wait()
    sky_load.wait()
    high = tab[0]
    left_table = jnp.concatenate([high[:size, :size], high[:size, size:]], axis=0)
    for c in range(n_chan):
        half = dot(left_table, sky_v[c]).astype(BF16)
        half = jnp.concatenate([half[:size], half[size:]], axis=1)
        full = dot(half, high).astype(BF16)
        spec[:size, c * size : (c + 1) * size] = full[:, :size]
        spec[size:, c * size : (c + 1) * size] = full[:, size:]

    row_ids = lax.broadcasted_iota(jnp.int32, (2 * size, lanes), 0) + 1
    group = 2 * slots
    groups = ((0, 1 + len(near), near), (1 + len(near), len(far), far))

    def answer(k, h):
        first, count, peers = groups[k]
        mat = place_mat[:, first * group : (first + count) * group]
        span = slice(h * per * size, (h + 1) * per * size)
        picked = dot_tn(mat, spec[:, span]).reshape(count, 2, 1, slots, per * size)
        picked = jnp.concatenate(
            [picked[..., c * size : (c + 1) * size] for c in range(per)], axis=2
        )
        row_send[h, first : first + count] = picked.reshape(count, per * group, size).astype(BF16)
        if k == 0:
            row_recv[h][0] = row_send[h, 0]
        exchange(row_send.at[h], row_recv[h], row_ssem.at[h], row_rsem.at[h], -1, peers)

    for k, (first, count, peers) in enumerate(groups):
        arrived(idx_recv.at[pl.ds(first + (k == 0), len(peers))], idx_rsem.at[k])
        span_k = slice(first * group, (first + count) * group)
        target = idx_recv[first, :, span_k]
        for e in range(first + 1, first + count):
            target = target + idx_recv[e, :, span_k]
        mat = jnp.where(row_ids[:, : count * group] == target, 1.0, 0.0).astype(BF16)
        place_mat[:, span_k] = mat
        answer(k, 0)
    for h in range(1, halves):
        for k in (1, 0):
            answer(k, h)

    rows_all = per * group
    n_vis = vt * size
    vis_load.wait()
    row_id = lax.broadcasted_iota(jnp.int32, (rows_all, n_vis), 0)
    vis_id = lax.broadcasted_iota(jnp.int32, (rows_all, n_vis), 1)
    live = (vis_id < count_s[0, 0]) & (row_id % vt == vis_id // size)
    first_slot = (row_id // vt) % nnz == 0
    first_out = (lax.broadcasted_iota(jnp.int32, (rows_all, 2 * size), 0) // vt) % nnz == 0
    for h in range(halves):
        con_buf[h, fpb] = jnp.zeros((rows_all, size), BF16)
    arrived(wv, local_sem.at[local_sem.shape[0] - 1])

    for h in range(halves):
        arrived(row_recv[h].at[pl.ds(1, nfx - 1)], row_rsem.at[h])
        measured = []
        for p in range(2):
            for c in range(per):
                both = vis_v[h * per + c].astype(F32)
                measured.append(jnp.broadcast_to(both[p : p + 1], (slots, n_vis)))
        measured = jnp.concatenate(measured, axis=0)
        sums = [None, None]
        for q in range(fpb // 2):
            x = jnp.concatenate(
                [row_recv[h][slot_s[2 * q]], row_recv[h][slot_s[2 * q + 1]]], axis=1
            )
            for n in range(nnz):
                term = dot_nt(x, wv[q, n].reshape(n_vis, 2 * size))
                sums[n] = term if sums[n] is None else sums[n] + term
        mixed = jnp.where(first_slot, sums[0], sums[1])
        later = pltpu.roll(mixed, rows_all - vt, 0)
        earlier = pltpu.roll(mixed, vt, 0)
        predicted = mixed + jnp.where(first_slot, later, earlier)
        residual = jnp.where(live, predicted - measured, 0.0).astype(BF16)
        for q in range(fpb // 2):
            terms = [dot(residual, wv[q, n].reshape(n_vis, 2 * size)) for n in range(nnz)]
            out = jnp.where(first_out, terms[0], terms[1]).astype(BF16)
            con_buf[h, 2 * q] = out[:, :size]
            con_buf[h, 2 * q + 1] = out[:, size:]
        for k in range(nfx):
            con_send[h, k] = con_buf[h, inv_s[k]]
        con_recv[h, 0] = con_send[h, 0]
        exchange(con_send.at[h], con_recv.at[h], con_ssem.at[h], con_rsem.at[h])

    def flipped(table):
        return jnp.concatenate(
            [
                jnp.concatenate([table[:size, :size], table[size:, :size]], axis=1),
                jnp.concatenate([table[:size, size:], table[size:, size:]], axis=1),
            ],
            axis=0,
        )

    right_back = (flipped(tab[0]), flipped(tab[1]))
    left_back = tuple(dot(tab[k, :size, :], place_mat[...]).astype(BF16) for k in range(2))
    lane_id = lax.broadcasted_iota(jnp.int32, (1, size), 1)
    quarter = size // 4
    block = 2 * (quarter + 32) + 2 * per * 16
    for h in range(halves):
        arrived(con_recv.at[h, pl.ds(1, nfx - 1)], con_rsem.at[h])
        own_rows = per * slots
        incoming = jnp.concatenate(
            [
                con_recv[h, :, p * own_rows : (p + 1) * own_rows, :].reshape(nfx * own_rows, size)
                for p in range(2)
            ],
            axis=1,
        )
        half = dot(incoming, right_back[0]) + dot(incoming, right_back[1])
        half = half.reshape(nfx, per, slots, 2 * size)
        half = jnp.concatenate(
            [
                jnp.concatenate(
                    [half[:, c : c + 1, :, p * size : (p + 1) * size] for p in range(2)], axis=1
                ).reshape(nfx * group, size)
                for c in range(per)
            ],
            axis=1,
        )
        grad = dot3(left_back, split(half))
        edges = [jnp.zeros((quarter, size), F32) for _ in range(2)]
        for c in range(per):
            stepped = sky_v[h * per + c].astype(F32) - STEP * grad[:, c * size : (c + 1) * size]
            shr[h * per + c] = stepped
            high = stepped.astype(BF16)
            st_bf[h, c] = high
            hi_buf[h, c, 16 : 16 + size, :size] = high
            for fold in range(4):
                at = 32 * fold + 16 * c
                part = stepped[fold * quarter : (fold + 1) * quarter]
                hit = (lane_id >= at) & (lane_id < at + 16)
                for e, turn in enumerate((at, (at + 16) % size)):
                    moved = pltpu.roll(part, turn, 1) if turn else part
                    edges[e] = jnp.where(hit, moved, edges[e])
        for e in range(2):
            edge_send[h, e] = edges[e].astype(BF16)

        first, last = pl.ds(0, 16), pl.ds(quarter - 16, 16)
        def send(src, at, count, device):
            pltpu.make_async_remote_copy(
                src_ref=src,
                dst_ref=halo_recv.at[h, pl.ds(at, count)],
                send_sem=halo_ssem.at[h],
                recv_sem=halo_rsem.at[h],
                device_id=device,
                device_id_type=MESH,
            ).start()

        for c in range(per):
            send(st_bf.at[h, c], c * size, size, mate)
        for who, where in ((0, blk), (1, 1 - blk)):
            fr = per * size + who * block
            fl, top = fr + quarter + 32, fr + 2 * (quarter + 32)
            bottom = top + per * 16
            send(edge_send.at[h, 0, first], fr + 16 + quarter, 16, (up, left, where))
            send(edge_send.at[h, 1, first], fl + 16 + quarter, 16, (up, right, where))
            send(edge_send.at[h, 0, last], fr, 16, (down, left, where))
            send(edge_send.at[h, 1, last], fl, 16, (down, right, where))
            send(edge_send.at[h, 0], fr + 16, quarter, (fy, left, where))
            send(edge_send.at[h, 1], fl + 16, quarter, (fy, right, where))
            for c in range(per):
                send(st_bf.at[h, c, pl.ds(0, 16)], bottom + 16 * c, 16, (up, fx, where))
                send(st_bf.at[h, c, pl.ds(size - 16, 16)], top + 16 * c, 16, (down, fx, where))

    tall = size + 32
    streams = 2 * per
    in_top, in_bottom = fy > 0, fy < nfy - 1
    row_tall = lax.broadcasted_iota(jnp.int32, (tall, 1), 0)
    rows_live = ((row_tall >= 16) | in_top) & ((row_tall < 16 + size) | in_bottom)
    zeros8 = jnp.zeros((8, size), F32)
    levels = thr_v.shape[0]
    thr_copy.wait_recv()
    for who, part in enumerate((thr_v, thr_mate)):
        for c in range(n_chan):
            for level in range(levels):
                at = (who * n_chan + c) * levels + level
                value = part[level : level + 1, c : c + 1]
                bounds[at : at + 1, :] = jnp.broadcast_to(value, (1, size))
    for buf in (ybuf, zbuf):
        for q in range(streams):
            for level in range(1, levels):
                buf[q, level, 0:8, :] = zeros8
                buf[q, level, 8 + tall : 16 + tall, :] = zeros8
    smooth_load.wait()
    thr_copy.wait_send()
    arrived(idx_send.at[pl.ds(1, nfx - 1)], idx_ssem.at[0])
    for h in range(halves):
        arrived(row_send.at[h, pl.ds(1, nfx - 1)], row_ssem.at[h])
        arrived(con_send.at[h, pl.ds(1, nfx - 1)], con_ssem.at[h])
    pieces = [(0, 0, 16, 3), (16 + size, 16 + quarter, 16, 0)]
    pieces += [(16 + k * quarter, 16, quarter, k) for k in range(4)]

    def summed(ref, at, count, s):
        x = ref[at : at + count, :]
        return (ref[at - s : at - s + count, :] + x) + (ref[at + s : at + s + count, :] + x)

    for h in range(halves):
        arrived(halo_recv.at[h], halo_rsem.at[h])
        for who in range(2):
            fr = per * size + who * block
            fl, top = fr + quarter + 32, fr + 2 * (quarter + 32)
            bottom = top + per * 16
            from_left = halo_recv[h, fl : fl + quarter + 32].astype(F32)
            from_right = halo_recv[h, fr : fr + quarter + 32].astype(F32)
            for c in range(per):
                q = who * per + c
                if who == 1:
                    hi_buf[h, q, 16 : 16 + size, :size] = halo_recv[h, c * size : (c + 1) * size]
                hi_buf[h, q, 0:16, :size] = jnp.where(
                    in_top, halo_recv[h, top + 16 * c : top + 16 * c + 16].astype(F32), 0.0
                ).astype(BF16)
                hi_buf[h, q, 16 + size :, :size] = jnp.where(
                    in_bottom, halo_recv[h, bottom + 16 * c : bottom + 16 * c + 16].astype(F32), 0.0
                ).astype(BF16)
                for to, start, count, fold in pieces:
                    at = 32 * fold + 16 * c
                    r = from_right[start : start + count]
                    r = pltpu.roll(r, size - at, 1) if at else r
                    l = pltpu.roll(from_left[start : start + count], (2 * size - 16 - at) % size, 1)
                    side = jnp.where(lane_id < 64, r, l)
                    if to in (0, 16 + size):
                        side = jnp.where(rows_live[to : to + count], side, 0.0)
                    hi_buf[h, q, to : to + count, size:] = side.astype(BF16)
        for t in range(levels // 2):
            span = slice(2 * t * size, 2 * (t + 1) * size)
            result = dot(hi_buf[h].reshape(streams * tall, 2 * size), smooth[:, span])
            for q in range(streams):
                for e in range(2):
                    ybuf[q, 2 * t + e, 8 : 8 + tall, :] = result[
                        q * tall : (q + 1) * tall, e * size : (e + 1) * size
                    ]
        for q in range(streams):
            who, c = q // per, h * per + q % per
            sources = [ybuf.at[q, 0]]
            for level in range(1, levels):
                source, dest = ybuf.at[q, level], zbuf.at[q, level]
                reach = 2 ** (level + 1) - 2
                for step in range(level):
                    s = 2**step
                    reach -= s if step else 0
                    low, top = (24 - reach) // 8 * 8, (24 + size + reach + 7) // 8 * 8
                    for at, stop in ((low, 24), (24 + size, top)):
                        part = summed(source, at, stop - at, s)
                        dest[at:stop, :] = jnp.where(rows_live[at - 8 : stop - 8], part, 0.0)
                    for at in range(24, 24 + size, 32):
                        dest[at : at + 32, :] = summed(source, at, 32, s)
                    source, dest = dest, source
                sources.append(source)
            for at in range(0, size, 16):
                rows = slice(at, at + 16)
                base = (q % per) * size + at
                value = shr[c, rows, :] if who == 0 else halo_recv[h, base : base + 16].astype(F32)
                coarse = value
                for level in range(levels):
                    at_bound = (who * n_chan + c) * levels + level
                    bound = bounds[at_bound : at_bound + 1, :]
                    finer = summed(sources[level], 24 + at, 16, 2**level)
                    value = value - jnp.minimum(jnp.maximum(coarse - finer, -bound), bound)
                    coarse = finer
                if who == 0:
                    shr[c, rows, :] = value
                else:
                    other[c, rows, :] = value

    for h in range(halves):
        arrived(halo_recv.at[h], halo_ssem.at[h])


def last_kernel(shr, other, mu_s, out_ref, gpart, gtot, xs):
    n_chan, size, _ = shr.shape
    total = 2 * n_chan
    chunk = 16
    pairs = [(a, b) for a in range(total) for b in range(a, total)]

    def step(i, sums):
        rows = pl.ds(pl.multiple_of(i * chunk, chunk), chunk)
        vals = [shr[c, rows, :] for c in range(n_chan)]
        vals += [other[c, rows, :].astype(F32) for c in range(n_chan)]
        news = []
        for k, (a, b) in enumerate(pairs):
            prod = vals[a] * vals[b]
            news.append(sums[k] + (prod[:8] + prod[8:]))
        return tuple(news)

    sums = lax.fori_loop(
        0, size // chunk, step, tuple(jnp.zeros((8, size), F32) for _ in pairs)
    )
    for (a, b), value in zip(pairs, sums):
        value = jnp.sum(value, axis=0, keepdims=True)
        gpart[a * total + b : a * total + b + 1, :] = value
        if a != b:
            gpart[b * total + a : b * total + a + 1, :] = value
    gtot[...] = jnp.broadcast_to(jnp.sum(gpart[...], axis=1, keepdims=True), gtot.shape)

    mu = mu_s[0] * float(size * size)
    mat = {}
    for a, b in pairs:
        value = jnp.broadcast_to(gtot[a * total + b : a * total + b + 1, :], (total, size))
        mat[a, b] = value + mu if a == b else value
    rhs = [gtot[c * total : (c + 1) * total, :] for c in range(total)]
    inverse = [None] * total
    for k in range(total):
        inverse[k] = 1.0 / mat[k, k]
        for i in range(k + 1, total):
            factor = mat[k, i] * inverse[k]
            for j in range(i, total):
                mat[i, j] = mat[i, j] - factor * mat[k, j]
            rhs[i] = rhs[i] - factor * rhs[k]
    solved = [None] * total
    for k in range(total - 1, -1, -1):
        value = rhs[k]
        for i in range(k + 1, total):
            value = value - mat[k, i] * solved[i]
        solved[k] = value * inverse[k]
        xs[k * total : (k + 1) * total, :] = solved[k]

    coeffs = [
        [jnp.broadcast_to(xs[c * total + d : c * total + d + 1, :], (8, size)) for c in range(total)]
        for d in range(n_chan)
    ]

    def finish(i, carry):
        rows = pl.ds(pl.multiple_of(i * chunk, chunk), chunk)
        vals = [shr[c, rows, :] for c in range(n_chan)]
        vals += [other[c, rows, :].astype(F32) for c in range(n_chan)]
        for d in range(n_chan):
            for h in range(2):
                value = coeffs[d][0] * vals[0][h * 8 : h * 8 + 8]
                for c in range(1, total):
                    value = value + coeffs[d][c] * vals[c][h * 8 : h * 8 + 8]
                out_ref[d, pl.ds(pl.multiple_of(i * chunk + h * 8, 8), 8), :] = value
        return carry

    lax.fori_loop(0, size // chunk, finish, 0)


def body(sizes, sky, vis, weights, tiles, lists, count, threshold, weight):
    nfx, nfy, nblk, fpb, vt, nnz, halves = sizes
    n_chan, size, _ = sky.shape
    per = n_chan // halves
    rows = per * 2 * vt * nnz
    lanes = nfx * 2 * vt * nnz
    hbm = pl.BlockSpec(memory_space=pltpu.HBM)
    smem = pl.BlockSpec(memory_space=pltpu.SMEM)
    vmem = pl.BlockSpec(memory_space=pltpu.VMEM)
    tall = size + 48
    levels = threshold.shape[0]
    sem = pltpu.SemaphoreType.DMA
    shr, other = pl.pallas_call(
        functools.partial(kernel, sizes),
        out_shape=[
            jax.ShapeDtypeStruct((n_chan, size, size), F32),
            jax.ShapeDtypeStruct((n_chan, size, size), F32),
        ],
        in_specs=[hbm] * 5 + [smem, hbm, hbm, hbm],
        out_specs=[vmem, vmem],
        scratch_shapes=[
            pltpu.SMEM((vt, nnz, fpb), jnp.int32),
            pltpu.SMEM((fpb,), jnp.int32),
            pltpu.VMEM((n_chan, size, size), BF16),
            pltpu.VMEM((n_chan, 2, vt * size), BF16),
            pltpu.VMEM((fpb // 2, nnz, vt, size, 2 * size), BF16),
            pltpu.VMEM((2, 2 * size, 2 * size), BF16),
            pltpu.VMEM((2 * size, levels * size), BF16),
            pltpu.VMEM((nfx, 1, lanes), jnp.int32),
            pltpu.VMEM((nfx, 1, lanes), jnp.int32),
            pltpu.VMEM((2 * size, n_chan * size), BF16),
            pltpu.VMEM((halves, nfx, rows, size), BF16),
            pltpu.VMEM((nfx, rows, size), BF16),
            pltpu.VMEM((nfx, rows, size), BF16),
            pltpu.VMEM((halves, fpb + 1, rows, size), BF16),
            pltpu.VMEM((halves, nfx, rows, size), BF16),
            pltpu.VMEM((halves, nfx, rows, size), BF16),
            pltpu.SMEM((nfx,), jnp.int32),
            pltpu.SMEM((fpb,), jnp.int32),
            pltpu.VMEM((2 * size, lanes), BF16),
            pltpu.VMEM((halves, per, size, size), BF16),
            pltpu.VMEM((halves, 2, size // 4, size), BF16),
            pltpu.VMEM((halves, per * size + 4 * (size // 4 + 32 + per * 16), size), BF16),
            pltpu.VMEM((halves, 2 * per, size + 32, 2 * size), BF16),
            pltpu.VMEM((2 * per, levels, tall, size), F32),
            pltpu.VMEM((2 * per, levels, tall, size), F32),
            pltpu.VMEM(threshold.shape, F32),
            pltpu.VMEM(threshold.shape, F32),
            pltpu.VMEM((2 * n_chan * levels, size), F32),
            sem((9,)),
            sem((1,)),
            sem((2,)),
            sem((halves,)),
            sem((halves,)),
            sem((halves,)),
            sem((halves,)),
            sem((halves,)),
            sem((halves,)),
            sem((2,)),
        ],
        compiler_params=pltpu.CompilerParams(
            collective_id=0, has_side_effects=True, vmem_limit_bytes=24 * 2**20
        ),
    )(
        pinned(sky),
        pinned(vis[0, 0]),
        pinned(weights[0, 0]),
        pinned(tiles[0, 0].transpose(1, 2, 0)),
        pinned(lists.reshape(-1)),
        count,
        pinned(threshold),
        pinned(jnp.asarray(tables(size))),
        pinned(jnp.asarray(smoothers(size, levels, 16))),
    )
    square = pltpu.VMEM((4 * n_chan * n_chan, size), F32)
    return pl.pallas_call(
        last_kernel,
        out_shape=jax.ShapeDtypeStruct((n_chan, size, size), F32),
        in_specs=[vmem, vmem, smem],
        out_specs=vmem,
        scratch_shapes=[square, square, square],
        compiler_params=pltpu.CompilerParams(vmem_limit_bytes=8 * 2**20),
    )(shr, other, weight.reshape(1))


def solution(mesh):
    in_specs = (
        P("blk", "fy", "fx"),
        P("fy", "fx", "blk", None, None),
        P("fy", "fx", None, None, None, None, None),
        P("fy", "fx", None, None, None),
        P("fy", "fx", None),
        P("fy", "fx"),
        P(None, "blk"),
        P(),
    )

    def step(*args):
        fpb, vt, nnz = args[3].shape[2:]
        sizes = (mesh.shape["fx"], mesh.shape["fy"], mesh.shape["blk"], fpb, vt, nnz, 2)
        return body(sizes, *args)

    return jax.shard_map(
        step, mesh=mesh, in_specs=in_specs, out_specs=P("blk", "fy", "fx"), check_vma=False
    )
```

```python
import functools
import math

import jax
import jax.numpy as jnp
import ml_dtypes
import numpy as np
from jax import lax
from jax.experimental import pallas as pl
from jax.experimental.pallas import tpu as pltpu
from jax.sharding import PartitionSpec as P

MESH = pl.DeviceIdType.MESH
F32 = jnp.float32
BF16 = jnp.bfloat16
STEP = 2.0


def tables(length):
    positions = np.arange(length)
    angles = (positions[:, None] * positions[None, :] % length) * (2.0 * math.pi / length)
    cosine = (np.cos(angles) / math.sqrt(length)).astype(np.float32)
    sinus = (np.sin(angles) / math.sqrt(length)).astype(np.float32)
    whole = np.concatenate(
        [np.concatenate([cosine, -sinus], axis=1), np.concatenate([sinus, cosine], axis=1)], axis=0
    )
    high = whole.astype(ml_dtypes.bfloat16)
    low = (whole - high.astype(np.float32)).astype(ml_dtypes.bfloat16)
    return np.stack([high, low])


def smoothers(size, levels, margin):
    reach = np.arange(-2 * margin, size + 2 * margin)
    apart = np.abs(reach[:, None] - reach[None, :])
    out = np.zeros((3, 2 * size, levels * size), np.float64)
    for variant in range(3):
        alive = np.ones(len(reach))
        if variant == 0:
            alive[reach < 0] = 0
        if variant == 2:
            alive[reach >= size] = 0
        whole = np.diag(alive)
        for level in range(levels):
            one = 2.0 * (apart == 0) + 1.0 * (apart == 2**level)
            whole = alive[:, None] * (one @ whole)
            taps = (whole / 16.0 ** (level + 1))[2 * margin : 2 * margin + size].T
            span = slice(level * size, (level + 1) * size)
            out[variant, :size, span] = taps[2 * margin : 2 * margin + size]
            out[variant, size : size + margin, span] = taps[2 * margin + size : 3 * margin + size]
            out[variant, 2 * size - margin :, span] = taps[margin : 2 * margin]
    return out.astype(ml_dtypes.bfloat16)


def dot(a, b):
    return jnp.dot(a, b, preferred_element_type=F32)


def dot_nt(a, b):
    return lax.dot_general(a, b, (((1,), (1,)), ((), ())), preferred_element_type=F32)


def dot_tn(a, b):
    return lax.dot_general(a, b, (((0,), (0,)), ((), ())), preferred_element_type=F32)


def split(values):
    high = values.astype(BF16)
    return high, (values - high.astype(F32)).astype(BF16)


def dot3(a, b):
    return dot(a[0], b[0]) + (dot(a[0], b[1]) + dot(a[1], b[0]))


def pinned(array):
    return pltpu.with_memory_space_constraint(array, pltpu.HBM)


def kernel(
    sizes,
    sky_hbm,
    vis_hbm,
    w_hbm,
    tiles_hbm,
    list_hbm,
    count_s,
    thr_hbm,
    tab_hbm,
    smooth_hbm,
    shr,
    other,
    tiles_s,
    list_s,
    sky_v,
    vis_v,
    wv,
    tab,
    smooth,
    idx_send,
    idx_recv,
    spec,
    row_send,
    row_recv0,
    row_recv1,
    con_buf,
    con_send,
    con_recv,
    inv_s,
    slot_s,
    place_mat,
    st_bf,
    edge_send,
    halo_recv,
    hi_buf,
    ybuf,
    zbuf,
    thr_v,
    thr_mate,
    bounds,
    local_sem,
    idx_ssem,
    idx_rsem,
    row_ssem,
    row_rsem,
    con_ssem,
    con_rsem,
    halo_ssem,
    halo_rsem,
    thr_sem,
):
    nfx, nfy, nblk, fpb, vt, nnz, halves = sizes
    n_chan, size, _ = sky_v.shape
    per = n_chan // halves
    row_recv = (row_recv0, row_recv1)
    slots = vt * nnz
    lanes = nfx * 2 * slots
    fy, fx, blk = lax.axis_index("fy"), lax.axis_index("fx"), lax.axis_index("blk")

    def along_fx(d):
        return (fy, lax.rem(fx + d, nfx), blk)

    up, down = lax.rem(fy + nfy - 1, nfy), lax.rem(fy + 1, nfy)
    left, right = lax.rem(fx + nfx - 1, nfx), lax.rem(fx + 1, nfx)
    mate = (fy, fx, 1 - blk)
    order = sorted(range(1, nfx), key=lambda d: -min(d, nfx - d))
    far = [d for d in order if min(d, nfx - d) > nfx // 4]
    near = [d for d in order if d not in far]
    slot = {d: k for k, d in enumerate([0] + near + far)}

    loads = []

    def arrived(buffer, semaphore):
        pltpu.make_async_copy(buffer, buffer, semaphore).wait()

    def load(src, dst):
        copy = pltpu.make_async_copy(src, dst, local_sem.at[len(loads)])
        copy.start()
        loads.append(copy)
        return copy

    barrier = pltpu.get_barrier_semaphore()
    others = [along_fx(d) for d in order]
    around = [(up, fx), (down, fx), (fy, left), (fy, right)]
    around += [(r, c) for r in (up, down) for c in (left, right)]
    others += [(up, fx, blk), (down, fx, blk), mate]
    others += [(r, c, blk) for r in (up, down) for c in (left, right)]
    others += [(r, c, 1 - blk) for r, c in around]
    for device in others:
        pl.semaphore_signal(barrier, inc=1, device_id=device, device_id_type=MESH)

    small_loads = [
        load(tiles_hbm, tiles_s),
        load(list_hbm, list_s),
    ]
    thr_load = load(thr_hbm, thr_v)
    tab_load = load(tab_hbm, tab)
    sky_load = load(sky_hbm, sky_v)
    vis_load = load(vis_hbm, vis_v)
    for f in range(fpb):
        for n in range(nnz):
            pltpu.make_async_copy(
                w_hbm.at[f, :, n],
                wv.at[f // 2, n, :, :, pl.ds((f % 2) * size, size)],
                local_sem.at[local_sem.shape[0] - 1],
            ).start()
    edge_kind = (fx + nfx - 2) // (nfx - 1) + fx // (nfx - 1)
    smooth_load = load(smooth_hbm.at[edge_kind], smooth)

    for copy in small_loads:
        copy.wait()
    lane = lax.broadcasted_iota(jnp.int32, (1, lanes), 1)
    lane_a, lane_n = lane % vt, (lane // vt) % nnz
    lane_p, lane_j = (lane // slots) % 2, lane // (2 * slots)
    wanted = []
    for f in range(fpb):
        row = jnp.zeros((1, lanes), jnp.int32)
        for a in range(vt):
            for n in range(nnz):
                here = (lane_a == a) & (lane_n == n)
                row = jnp.where(here, tiles_s[a, n, f], row)
        wanted.append(row + lane_p * size + 1)
    where_f = [0] * fpb
    for d in range(nfx):
        owner = lax.rem(fx + d, nfx)
        request = jnp.zeros((1, lanes), jnp.int32)
        place = fpb
        for f in range(fpb):
            hit = list_s[f] == owner
            request = jnp.where(hit, wanted[f], request)
            place = jnp.where(hit, f, place)
            where_f[f] = jnp.where(hit, slot[d], where_f[f])
        idx_send[slot[d]] = jnp.where(lane_j == slot[d], request, 0)
        inv_s[slot[d]] = place
    for f in range(fpb):
        slot_s[f] = where_f[f]
    idx_recv[0] = idx_send[0]

    pl.semaphore_wait(barrier, len(others))

    def exchange(send, recv, ssem, rsem, sign=1, peers=order):
        for d in peers:
            pltpu.make_async_remote_copy(
                src_ref=send.at[slot[d]],
                dst_ref=recv.at[slot[d]],
                send_sem=ssem,
                recv_sem=rsem if peers is order or sign < 0 else rsem.at[int(d in far)],
                device_id=along_fx(d if sign > 0 else nfx - d),
                device_id_type=MESH,
            ).start()

    exchange(idx_send, idx_recv, idx_ssem.at[0], idx_rsem, 1, far)
    exchange(idx_send, idx_recv, idx_ssem.at[0], idx_rsem, 1, near)
    thr_load.wait()
    thr_copy = pltpu.make_async_remote_copy(
        src_ref=thr_v,
        dst_ref=thr_mate,
        send_sem=thr_sem.at[0],
        recv_sem=thr_sem.at[1],
        device_id=mate,
        device_id_type=MESH,
    )
    thr_copy.start()

    tab_load.wait()
    sky_load.wait()
    high = tab[0]
    left_table = jnp.concatenate([high[:size, :size], high[:size, size:]], axis=0)
    for c in range(n_chan):
        half = dot(left_table, sky_v[c]).astype(BF16)
        half = jnp.concatenate([half[:size], half[size:]], axis=1)
        full = dot(half, high).astype(BF16)
        spec[:size, c * size : (c + 1) * size] = full[:, :size]
        spec[size:, c * size : (c + 1) * size] = full[:, size:]

    row_ids = lax.broadcasted_iota(jnp.int32, (2 * size, lanes), 0) + 1
    group = 2 * slots
    groups = ((0, 1 + len(near), near), (1 + len(near), len(far), far))

    def answer(k, h):
        first, count, peers = groups[k]
        mat = place_mat[:, first * group : (first + count) * group]
        span = slice(h * per * size, (h + 1) * per * size)
        picked = dot_tn(mat, spec[:, span]).reshape(count, 2, 1, slots, per * size)
        picked = jnp.concatenate(
            [picked[..., c * size : (c + 1) * size] for c in range(per)], axis=2
        )
        row_send[h, first : first + count] = picked.reshape(count, per * group, size).astype(BF16)
        if k == 0:
            row_recv[h][0] = row_send[h, 0]
        exchange(row_send.at[h], row_recv[h], row_ssem.at[h], row_rsem.at[h], -1, peers)

    for k, (first, count, peers) in enumerate(groups):
        arrived(idx_recv.at[pl.ds(first + (k == 0), len(peers))], idx_rsem.at[k])
        span_k = slice(first * group, (first + count) * group)
        target = idx_recv[first, :, span_k]
        for e in range(first + 1, first + count):
            target = target + idx_recv[e, :, span_k]
        mat = jnp.where(row_ids[:, : count * group] == target, 1.0, 0.0).astype(BF16)
        place_mat[:, span_k] = mat
        answer(k, 0)
    for h in range(1, halves):
        for k in (1, 0):
            answer(k, h)

    rows_all = per * group
    n_vis = vt * size
    vis_load.wait()
    row_id = lax.broadcasted_iota(jnp.int32, (rows_all, n_vis), 0)
    vis_id = lax.broadcasted_iota(jnp.int32, (rows_all, n_vis), 1)
    live = (vis_id < count_s[0, 0]) & (row_id % vt == vis_id // size)
    first_slot = (row_id // vt) % nnz == 0
    first_out = (lax.broadcasted_iota(jnp.int32, (rows_all, 2 * size), 0) // vt) % nnz == 0
    for h in range(halves):
        con_buf[h, fpb] = jnp.zeros((rows_all, size), BF16)
    arrived(wv, local_sem.at[local_sem.shape[0] - 1])

    for h in range(halves):
        arrived(row_recv[h].at[pl.ds(1, nfx - 1)], row_rsem.at[h])
        measured = []
        for p in range(2):
            for c in range(per):
                both = vis_v[h * per + c].astype(F32)
                measured.append(jnp.broadcast_to(both[p : p + 1], (slots, n_vis)))
        measured = jnp.concatenate(measured, axis=0)
        sums = [None, None]
        for q in range(fpb // 2):
            x = jnp.concatenate(
                [row_recv[h][slot_s[2 * q]], row_recv[h][slot_s[2 * q + 1]]], axis=1
            )
            for n in range(nnz):
                term = dot_nt(x, wv[q, n].reshape(n_vis, 2 * size))
                sums[n] = term if sums[n] is None else sums[n] + term
        mixed = jnp.where(first_slot, sums[0], sums[1])
        later = pltpu.roll(mixed, rows_all - vt, 0)
        earlier = pltpu.roll(mixed, vt, 0)
        predicted = mixed + jnp.where(first_slot, later, earlier)
        residual = jnp.where(live, predicted - measured, 0.0).astype(BF16)
        for q in range(fpb // 2):
            terms = [dot(residual, wv[q, n].reshape(n_vis, 2 * size)) for n in range(nnz)]
            out = jnp.where(first_out, terms[0], terms[1]).astype(BF16)
            con_buf[h, 2 * q] = out[:, :size]
            con_buf[h, 2 * q + 1] = out[:, size:]
        for k in range(nfx):
            con_send[h, k] = con_buf[h, inv_s[k]]
        con_recv[h, 0] = con_send[h, 0]
        exchange(con_send.at[h], con_recv.at[h], con_ssem.at[h], con_rsem.at[h])

    def flipped(table):
        return jnp.concatenate(
            [
                jnp.concatenate([table[:size, :size], table[size:, :size]], axis=1),
                jnp.concatenate([table[:size, size:], table[size:, size:]], axis=1),
            ],
            axis=0,
        )

    right_back = (flipped(tab[0]), flipped(tab[1]))
    left_back = tuple(dot(tab[k, :size, :], place_mat[...]).astype(BF16) for k in range(2))
    lane_id = lax.broadcasted_iota(jnp.int32, (1, size), 1)
    quarter = size // 4
    block = 2 * (quarter + 32) + 2 * per * 16
    for h in range(halves):
        arrived(con_recv.at[h, pl.ds(1, nfx - 1)], con_rsem.at[h])
        own_rows = per * slots
        incoming = jnp.concatenate(
            [
                con_recv[h, :, p * own_rows : (p + 1) * own_rows, :].reshape(nfx * own_rows, size)
                for p in range(2)
            ],
            axis=1,
        )
        half = dot(incoming, right_back[0]) + dot(incoming, right_back[1])
        half = half.reshape(nfx, per, slots, 2 * size)
        half = jnp.concatenate(
            [
                jnp.concatenate(
                    [half[:, c : c + 1, :, p * size : (p + 1) * size] for p in range(2)], axis=1
                ).reshape(nfx * group, size)
                for c in range(per)
            ],
            axis=1,
        )
        grad = dot3(left_back, split(half))
        edges = [jnp.zeros((quarter, size), F32) for _ in range(2)]
        for c in range(per):
            stepped = sky_v[h * per + c].astype(F32) - STEP * grad[:, c * size : (c + 1) * size]
            shr[h * per + c] = stepped
            high = stepped.astype(BF16)
            st_bf[h, c] = high
            hi_buf[h, c, 16 : 16 + size, :size] = high
            for fold in range(4):
                at = 32 * fold + 16 * c
                part = stepped[fold * quarter : (fold + 1) * quarter]
                hit = (lane_id >= at) & (lane_id < at + 16)
                for e, turn in enumerate((at, (at + 16) % size)):
                    moved = pltpu.roll(part, turn, 1) if turn else part
                    edges[e] = jnp.where(hit, moved, edges[e])
        for e in range(2):
            edge_send[h, e] = edges[e].astype(BF16)

        first, last = pl.ds(0, 16), pl.ds(quarter - 16, 16)
        def send(src, at, count, device):
            pltpu.make_async_remote_copy(
                src_ref=src,
                dst_ref=halo_recv.at[h, pl.ds(at, count)],
                send_sem=halo_ssem.at[h],
                recv_sem=halo_rsem.at[h],
                device_id=device,
                device_id_type=MESH,
            ).start()

        for who, where in ((0, blk), (1, 1 - blk)):
            fr = per * size + who * block
            fl, top = fr + quarter + 32, fr + 2 * (quarter + 32)
            bottom = top + per * 16
            send(edge_send.at[h, 0, first], fr + 16 + quarter, 16, (up, left, where))
            send(edge_send.at[h, 1, first], fl + 16 + quarter, 16, (up, right, where))
            send(edge_send.at[h, 0, last], fr, 16, (down, left, where))
            send(edge_send.at[h, 1, last], fl, 16, (down, right, where))
            send(edge_send.at[h, 0], fr + 16, quarter, (fy, left, where))
            send(edge_send.at[h, 1], fl + 16, quarter, (fy, right, where))
            for c in range(per):
                send(st_bf.at[h, c, pl.ds(0, 16)], bottom + 16 * c, 16, (up, fx, where))
                send(st_bf.at[h, c, pl.ds(size - 16, 16)], top + 16 * c, 16, (down, fx, where))
        for c in range(per):
            send(st_bf.at[h, c], c * size, size, mate)

    tall = size + 32
    streams = 2 * per
    in_top, in_bottom = fy > 0, fy < nfy - 1
    row_tall = lax.broadcasted_iota(jnp.int32, (tall, 1), 0)
    rows_live = ((row_tall >= 16) | in_top) & ((row_tall < 16 + size) | in_bottom)
    zeros8 = jnp.zeros((8, size), F32)
    levels = thr_v.shape[0]
    thr_copy.wait_recv()
    for who, part in enumerate((thr_v, thr_mate)):
        for c in range(n_chan):
            for level in range(levels):
                at = (who * n_chan + c) * levels + level
                value = part[level : level + 1, c : c + 1]
                bounds[at : at + 1, :] = jnp.broadcast_to(value, (1, size))
    for buf in (ybuf, zbuf):
        for q in range(streams):
            for level in range(1, levels):
                buf[q, level, 0:8, :] = zeros8
                buf[q, level, 8 + tall : 16 + tall, :] = zeros8
    smooth_load.wait()
    thr_copy.wait_send()
    arrived(idx_send.at[pl.ds(1, nfx - 1)], idx_ssem.at[0])
    for h in range(halves):
        arrived(row_send.at[h, pl.ds(1, nfx - 1)], row_ssem.at[h])
        arrived(con_send.at[h, pl.ds(1, nfx - 1)], con_ssem.at[h])
    pieces = [(0, 0, 16, 3), (16 + size, 16 + quarter, 16, 0)]
    pieces += [(16 + k * quarter, 16, quarter, k) for k in range(4)]

    def summed(ref, at, count, s):
        x = ref[at : at + count, :]
        return (ref[at - s : at - s + count, :] + x) + (ref[at + s : at + s + count, :] + x)

    for h in range(halves):
        arrived(halo_recv.at[h], halo_rsem.at[h])
        for who in range(2):
            fr = per * size + who * block
            fl, top = fr + quarter + 32, fr + 2 * (quarter + 32)
            bottom = top + per * 16
            from_left = halo_recv[h, fl : fl + quarter + 32].astype(F32)
            from_right = halo_recv[h, fr : fr + quarter + 32].astype(F32)
            for c in range(per):
                q = who * per + c
                if who == 1:
                    hi_buf[h, q, 16 : 16 + size, :size] = halo_recv[h, c * size : (c + 1) * size]
                hi_buf[h, q, 0:16, :size] = jnp.where(
                    in_top, halo_recv[h, top + 16 * c : top + 16 * c + 16].astype(F32), 0.0
                ).astype(BF16)
                hi_buf[h, q, 16 + size :, :size] = jnp.where(
                    in_bottom, halo_recv[h, bottom + 16 * c : bottom + 16 * c + 16].astype(F32), 0.0
                ).astype(BF16)
                for to, start, count, fold in pieces:
                    at = 32 * fold + 16 * c
                    r = from_right[start : start + count]
                    r = pltpu.roll(r, size - at, 1) if at else r
                    l = pltpu.roll(from_left[start : start + count], (2 * size - 16 - at) % size, 1)
                    side = jnp.where(lane_id < 64, r, l)
                    if to in (0, 16 + size):
                        side = jnp.where(rows_live[to : to + count], side, 0.0)
                    hi_buf[h, q, to : to + count, size:] = side.astype(BF16)
        for t in range(levels // 2):
            span = slice(2 * t * size, 2 * (t + 1) * size)
            result = dot(hi_buf[h].reshape(streams * tall, 2 * size), smooth[:, span])
            for q in range(streams):
                for e in range(2):
                    ybuf[q, 2 * t + e, 8 : 8 + tall, :] = result[
                        q * tall : (q + 1) * tall, e * size : (e + 1) * size
                    ]
        for q in range(streams):
            who, c = q // per, h * per + q % per
            sources = [ybuf.at[q, 0]]
            for level in range(1, levels):
                source, dest = ybuf.at[q, level], zbuf.at[q, level]
                reach = 2 ** (level + 1) - 2
                for step in range(level):
                    s = 2**step
                    reach -= s if step else 0
                    low, top = (24 - reach) // 8 * 8, (24 + size + reach + 7) // 8 * 8
                    for at, stop in ((low, 24), (24 + size, top)):
                        part = summed(source, at, stop - at, s)
                        dest[at:stop, :] = jnp.where(rows_live[at - 8 : stop - 8], part, 0.0)
                    for at in range(24, 24 + size, 32):
                        dest[at : at + 32, :] = summed(source, at, 32, s)
                    source, dest = dest, source
                sources.append(source)
            for at in range(0, size, 16):
                rows = slice(at, at + 16)
                base = (q % per) * size + at
                value = shr[c, rows, :] if who == 0 else halo_recv[h, base : base + 16].astype(F32)
                coarse = value
                for level in range(levels):
                    at_bound = (who * n_chan + c) * levels + level
                    bound = bounds[at_bound : at_bound + 1, :]
                    finer = summed(sources[level], 24 + at, 16, 2**level)
                    value = value - jnp.minimum(jnp.maximum(coarse - finer, -bound), bound)
                    coarse = finer
                if who == 0:
                    shr[c, rows, :] = value
                else:
                    other[c, rows, :] = value

    for h in range(halves):
        arrived(halo_recv.at[h], halo_ssem.at[h])


def last_kernel(shr, other, mu_s, out_hbm, out_ref, gpart, gtot, xs, out_sem):
    n_chan, size, _ = shr.shape
    total = 2 * n_chan
    chunk = 16
    pairs = [(a, b) for a in range(total) for b in range(a, total)]

    def step(i, sums):
        rows = pl.ds(pl.multiple_of(i * chunk, chunk), chunk)
        vals = [shr[c, rows, :] for c in range(n_chan)]
        vals += [other[c, rows, :].astype(F32) for c in range(n_chan)]
        news = []
        for k, (a, b) in enumerate(pairs):
            prod = vals[a] * vals[b]
            news.append(sums[k] + (prod[:8] + prod[8:]))
        return tuple(news)

    sums = lax.fori_loop(
        0, size // chunk, step, tuple(jnp.zeros((8, size), F32) for _ in pairs)
    )
    for (a, b), value in zip(pairs, sums):
        value = jnp.sum(value, axis=0, keepdims=True)
        gpart[a * total + b : a * total + b + 1, :] = value
        if a != b:
            gpart[b * total + a : b * total + a + 1, :] = value
    gtot[...] = jnp.broadcast_to(jnp.sum(gpart[...], axis=1, keepdims=True), gtot.shape)

    mu = mu_s[0] * float(size * size)
    mat = {}
    for a, b in pairs:
        value = jnp.broadcast_to(gtot[a * total + b : a * total + b + 1, :], (total, size))
        mat[a, b] = value + mu if a == b else value
    rhs = [gtot[c * total : (c + 1) * total, :] for c in range(total)]
    inverse = [None] * total
    for k in range(total):
        inverse[k] = 1.0 / mat[k, k]
        for i in range(k + 1, total):
            factor = mat[k, i] * inverse[k]
            for j in range(i, total):
                mat[i, j] = mat[i, j] - factor * mat[k, j]
            rhs[i] = rhs[i] - factor * rhs[k]
    solved = [None] * total
    for k in range(total - 1, -1, -1):
        value = rhs[k]
        for i in range(k + 1, total):
            value = value - mat[k, i] * solved[i]
        solved[k] = value * inverse[k]
        xs[k * total : (k + 1) * total, :] = solved[k]

    coeffs = [
        [jnp.broadcast_to(xs[c * total + d : c * total + d + 1, :], (8, size)) for c in range(total)]
        for d in range(n_chan)
    ]

    def finish(i, carry):
        rows = pl.ds(pl.multiple_of(i * chunk, chunk), chunk)
        vals = [shr[c, rows, :] for c in range(n_chan)]
        vals += [other[c, rows, :].astype(F32) for c in range(n_chan)]
        for d in range(n_chan):
            for h in range(2):
                value = coeffs[d][0] * vals[0][h * 8 : h * 8 + 8]
                for c in range(1, total):
                    value = value + coeffs[d][c] * vals[c][h * 8 : h * 8 + 8]
                out_ref[d, pl.ds(pl.multiple_of(i * chunk + h * 8, 8), 8), :] = value
        return carry

    parts = 4
    each = size // chunk // parts
    copies = []
    for part in range(parts):
        lax.fori_loop(part * each, (part + 1) * each, finish, 0)
        rows = pl.ds(part * each * chunk, each * chunk)
        copy = pltpu.make_async_copy(
            out_ref.at[:, rows, :], out_hbm.at[:, rows, :], out_sem.at[part]
        )
        copy.start()
        copies.append(copy)
    for copy in copies:
        copy.wait()


def body(sizes, sky, vis, weights, tiles, lists, count, threshold, weight):
    nfx, nfy, nblk, fpb, vt, nnz, halves = sizes
    n_chan, size, _ = sky.shape
    per = n_chan // halves
    rows = per * 2 * vt * nnz
    lanes = nfx * 2 * vt * nnz
    hbm = pl.BlockSpec(memory_space=pltpu.HBM)
    smem = pl.BlockSpec(memory_space=pltpu.SMEM)
    vmem = pl.BlockSpec(memory_space=pltpu.VMEM)
    tall = size + 48
    levels = threshold.shape[0]
    sem = pltpu.SemaphoreType.DMA
    shr, other = pl.pallas_call(
        functools.partial(kernel, sizes),
        out_shape=[
            jax.ShapeDtypeStruct((n_chan, size, size), F32),
            jax.ShapeDtypeStruct((n_chan, size, size), F32),
        ],
        in_specs=[hbm] * 5 + [smem, hbm, hbm, hbm],
        out_specs=[vmem, vmem],
        scratch_shapes=[
            pltpu.SMEM((vt, nnz, fpb), jnp.int32),
            pltpu.SMEM((fpb,), jnp.int32),
            pltpu.VMEM((n_chan, size, size), BF16),
            pltpu.VMEM((n_chan, 2, vt * size), BF16),
            pltpu.VMEM((fpb // 2, nnz, vt, size, 2 * size), BF16),
            pltpu.VMEM((2, 2 * size, 2 * size), BF16),
            pltpu.VMEM((2 * size, levels * size), BF16),
            pltpu.VMEM((nfx, 1, lanes), jnp.int32),
            pltpu.VMEM((nfx, 1, lanes), jnp.int32),
            pltpu.VMEM((2 * size, n_chan * size), BF16),
            pltpu.VMEM((halves, nfx, rows, size), BF16),
            pltpu.VMEM((nfx, rows, size), BF16),
            pltpu.VMEM((nfx, rows, size), BF16),
            pltpu.VMEM((halves, fpb + 1, rows, size), BF16),
            pltpu.VMEM((halves, nfx, rows, size), BF16),
            pltpu.VMEM((halves, nfx, rows, size), BF16),
            pltpu.SMEM((nfx,), jnp.int32),
            pltpu.SMEM((fpb,), jnp.int32),
            pltpu.VMEM((2 * size, lanes), BF16),
            pltpu.VMEM((halves, per, size, size), BF16),
            pltpu.VMEM((halves, 2, size // 4, size), BF16),
            pltpu.VMEM((halves, per * size + 4 * (size // 4 + 32 + per * 16), size), BF16),
            pltpu.VMEM((halves, 2 * per, size + 32, 2 * size), BF16),
            pltpu.VMEM((2 * per, levels, tall, size), F32),
            pltpu.VMEM((2 * per, levels, tall, size), F32),
            pltpu.VMEM(threshold.shape, F32),
            pltpu.VMEM(threshold.shape, F32),
            pltpu.VMEM((2 * n_chan * levels, size), F32),
            sem((9,)),
            sem((1,)),
            sem((2,)),
            sem((halves,)),
            sem((halves,)),
            sem((halves,)),
            sem((halves,)),
            sem((halves,)),
            sem((halves,)),
            sem((2,)),
        ],
        compiler_params=pltpu.CompilerParams(
            collective_id=0, has_side_effects=True, vmem_limit_bytes=24 * 2**20
        ),
    )(
        pinned(sky),
        pinned(vis[0, 0]),
        pinned(weights[0, 0]),
        pinned(tiles[0, 0].transpose(1, 2, 0)),
        pinned(lists.reshape(-1)),
        count,
        pinned(threshold),
        pinned(jnp.asarray(tables(size))),
        pinned(jnp.asarray(smoothers(size, levels, 16))),
    )
    square = pltpu.VMEM((4 * n_chan * n_chan, size), F32)
    return pl.pallas_call(
        last_kernel,
        out_shape=jax.ShapeDtypeStruct((n_chan, size, size), F32),
        in_specs=[vmem, vmem, smem],
        out_specs=hbm,
        scratch_shapes=[pltpu.VMEM((n_chan, size, size), F32), square, square, square, sem((4,))],
        compiler_params=pltpu.CompilerParams(vmem_limit_bytes=8 * 2**20),
    )(shr, other, weight.reshape(1))


def solution(mesh):
    in_specs = (
        P("blk", "fy", "fx"),
        P("fy", "fx", "blk", None, None),
        P("fy", "fx", None, None, None, None, None),
        P("fy", "fx", None, None, None),
        P("fy", "fx", None),
        P("fy", "fx"),
        P(None, "blk"),
        P(),
    )

    def step(*args):
        fpb, vt, nnz = args[3].shape[2:]
        sizes = (mesh.shape["fx"], mesh.shape["fy"], mesh.shape["blk"], fpb, vt, nnz, 2)
        return body(sizes, *args)

    return jax.shard_map(
        step, mesh=mesh, in_specs=in_specs, out_specs=P("blk", "fy", "fx"), check_vma=False
    )
```

```python
import functools
import math

import jax
import jax.numpy as jnp
import ml_dtypes
import numpy as np
from jax import lax
from jax.experimental import pallas as pl
from jax.experimental.pallas import tpu as pltpu
from jax.sharding import PartitionSpec as P

MESH = pl.DeviceIdType.MESH
F32 = jnp.float32
BF16 = jnp.bfloat16
STEP = 2.0


def tables(length):
    positions = np.arange(length)
    angles = (positions[:, None] * positions[None, :] % length) * (2.0 * math.pi / length)
    cosine = (np.cos(angles) / math.sqrt(length)).astype(np.float32)
    sinus = (np.sin(angles) / math.sqrt(length)).astype(np.float32)
    whole = np.concatenate(
        [np.concatenate([cosine, -sinus], axis=1), np.concatenate([sinus, cosine], axis=1)], axis=0
    )
    high = whole.astype(ml_dtypes.bfloat16)
    low = (whole - high.astype(np.float32)).astype(ml_dtypes.bfloat16)
    return np.stack([high, low])


def smoothers(size, levels, margin):
    reach = np.arange(-2 * margin, size + 2 * margin)
    apart = np.abs(reach[:, None] - reach[None, :])
    out = np.zeros((3, 2 * size, levels * size), np.float64)
    for variant in range(3):
        alive = np.ones(len(reach))
        if variant == 0:
            alive[reach < 0] = 0
        if variant == 2:
            alive[reach >= size] = 0
        whole = np.diag(alive)
        for level in range(levels):
            one = 2.0 * (apart == 0) + 1.0 * (apart == 2**level)
            whole = alive[:, None] * (one @ whole)
            taps = (whole / 16.0 ** (level + 1))[2 * margin : 2 * margin + size].T
            span = slice(level * size, (level + 1) * size)
            out[variant, :size, span] = taps[2 * margin : 2 * margin + size]
            out[variant, size : size + margin, span] = taps[2 * margin + size : 3 * margin + size]
            out[variant, 2 * size - margin :, span] = taps[margin : 2 * margin]
    return out.astype(ml_dtypes.bfloat16)


def dot(a, b):
    return jnp.dot(a, b, preferred_element_type=F32)


def dot_nt(a, b):
    return lax.dot_general(a, b, (((1,), (1,)), ((), ())), preferred_element_type=F32)


def dot_tn(a, b):
    return lax.dot_general(a, b, (((0,), (0,)), ((), ())), preferred_element_type=F32)


def split(values):
    high = values.astype(BF16)
    return high, (values - high.astype(F32)).astype(BF16)


def dot3(a, b):
    return dot(a[0], b[0]) + (dot(a[0], b[1]) + dot(a[1], b[0]))


def pinned(array):
    return pltpu.with_memory_space_constraint(array, pltpu.HBM)


def kernel(
    sizes,
    sky_hbm,
    vis_hbm,
    w_hbm,
    tiles_hbm,
    list_hbm,
    count_s,
    thr_hbm,
    tab_hbm,
    smooth_hbm,
    shr,
    other,
    tiles_s,
    list_s,
    sky_v,
    vis_v,
    wv,
    tab,
    smooth,
    idx_send,
    idx_recv,
    spec,
    row_send,
    row_recv0,
    row_recv1,
    con_buf,
    con_send,
    con_recv,
    inv_s,
    slot_s,
    place_mat,
    st_bf,
    edge_send,
    halo_recv,
    hi_buf,
    ybuf,
    zbuf,
    thr_v,
    thr_mate,
    bounds,
    local_sem,
    idx_ssem,
    idx_rsem,
    row_ssem,
    row_rsem,
    con_ssem,
    con_rsem,
    halo_ssem,
    halo_rsem,
    thr_sem,
):
    nfx, nfy, nblk, fpb, vt, nnz, halves = sizes
    n_chan, size, _ = sky_v.shape
    per = n_chan // halves
    row_recv = (row_recv0, row_recv1)
    slots = vt * nnz
    lanes = nfx * 2 * slots
    fy, fx, blk = lax.axis_index("fy"), lax.axis_index("fx"), lax.axis_index("blk")

    def along_fx(d):
        return (fy, lax.rem(fx + d, nfx), blk)

    up, down = lax.rem(fy + nfy - 1, nfy), lax.rem(fy + 1, nfy)
    left, right = lax.rem(fx + nfx - 1, nfx), lax.rem(fx + 1, nfx)
    mate = (fy, fx, 1 - blk)
    order = sorted(range(1, nfx), key=lambda d: -min(d, nfx - d))
    far = [d for d in order if min(d, nfx - d) > 3 * nfx // 8]
    near = [d for d in order if d not in far]
    slot = {d: k for k, d in enumerate([0] + near + far)}

    loads = []

    def arrived(buffer, semaphore):
        pltpu.make_async_copy(buffer, buffer, semaphore).wait()

    def load(src, dst):
        copy = pltpu.make_async_copy(src, dst, local_sem.at[len(loads)])
        copy.start()
        loads.append(copy)
        return copy

    barrier = pltpu.get_barrier_semaphore()
    others = [along_fx(d) for d in order]
    around = [(up, fx), (down, fx), (fy, left), (fy, right)]
    around += [(r, c) for r in (up, down) for c in (left, right)]
    others += [(up, fx, blk), (down, fx, blk), mate]
    others += [(r, c, blk) for r in (up, down) for c in (left, right)]
    others += [(r, c, 1 - blk) for r, c in around]
    for device in others:
        pl.semaphore_signal(barrier, inc=1, device_id=device, device_id_type=MESH)

    small_loads = [
        load(tiles_hbm, tiles_s),
        load(list_hbm, list_s),
    ]
    thr_load = load(thr_hbm, thr_v)
    tab_load = load(tab_hbm, tab)
    sky_load = load(sky_hbm, sky_v)
    vis_load = load(vis_hbm, vis_v)
    for f in range(fpb):
        for n in range(nnz):
            pltpu.make_async_copy(
                w_hbm.at[f, :, n],
                wv.at[f // 2, n, :, :, pl.ds((f % 2) * size, size)],
                local_sem.at[local_sem.shape[0] - 1],
            ).start()
    edge_kind = (fx + nfx - 2) // (nfx - 1) + fx // (nfx - 1)
    smooth_load = load(smooth_hbm.at[edge_kind], smooth)

    for copy in small_loads:
        copy.wait()
    lane = lax.broadcasted_iota(jnp.int32, (1, lanes), 1)
    lane_a, lane_n = lane % vt, (lane // vt) % nnz
    lane_p, lane_j = (lane // slots) % 2, lane // (2 * slots)
    wanted = []
    for f in range(fpb):
        row = jnp.zeros((1, lanes), jnp.int32)
        for a in range(vt):
            for n in range(nnz):
                here = (lane_a == a) & (lane_n == n)
                row = jnp.where(here, tiles_s[a, n, f], row)
        wanted.append(row + lane_p * size + 1)
    where_f = [0] * fpb
    for d in range(nfx):
        owner = lax.rem(fx + d, nfx)
        request = jnp.zeros((1, lanes), jnp.int32)
        place = fpb
        for f in range(fpb):
            hit = list_s[f] == owner
            request = jnp.where(hit, wanted[f], request)
            place = jnp.where(hit, f, place)
            where_f[f] = jnp.where(hit, slot[d], where_f[f])
        idx_send[slot[d]] = jnp.where(lane_j == slot[d], request, 0)
        inv_s[slot[d]] = place
    for f in range(fpb):
        slot_s[f] = where_f[f]
    idx_recv[0] = idx_send[0]

    pl.semaphore_wait(barrier, len(others))

    def exchange(send, recv, ssem, rsem, sign=1, peers=order):
        for d in peers:
            pltpu.make_async_remote_copy(
                src_ref=send.at[slot[d]],
                dst_ref=recv.at[slot[d]],
                send_sem=ssem,
                recv_sem=rsem if peers is order or sign < 0 else rsem.at[int(d in far)],
                device_id=along_fx(d if sign > 0 else nfx - d),
                device_id_type=MESH,
            ).start()

    exchange(idx_send, idx_recv, idx_ssem.at[0], idx_rsem, 1, far)
    exchange(idx_send, idx_recv, idx_ssem.at[0], idx_rsem, 1, near)
    thr_load.wait()
    thr_copy = pltpu.make_async_remote_copy(
        src_ref=thr_v,
        dst_ref=thr_mate,
        send_sem=thr_sem.at[0],
        recv_sem=thr_sem.at[1],
        device_id=mate,
        device_id_type=MESH,
    )
    thr_copy.start()

    tab_load.wait()
    sky_load.wait()
    high = tab[0]
    left_table = jnp.concatenate([high[:size, :size], high[:size, size:]], axis=0)
    for c in range(n_chan):
        half = dot(left_table, sky_v[c]).astype(BF16)
        half = jnp.concatenate([half[:size], half[size:]], axis=1)
        full = dot(half, high).astype(BF16)
        spec[:size, c * size : (c + 1) * size] = full[:, :size]
        spec[size:, c * size : (c + 1) * size] = full[:, size:]

    row_ids = lax.broadcasted_iota(jnp.int32, (2 * size, lanes), 0) + 1
    group = 2 * slots
    groups = ((0, 1 + len(near), near), (1 + len(near), len(far), far))

    def answer(k, h):
        first, count, peers = groups[k]
        mat = place_mat[:, first * group : (first + count) * group]
        span = slice(h * per * size, (h + 1) * per * size)
        picked = dot_tn(mat, spec[:, span]).reshape(count, 2, 1, slots, per * size)
        picked = jnp.concatenate(
            [picked[..., c * size : (c + 1) * size] for c in range(per)], axis=2
        )
        row_send[h, first : first + count] = picked.reshape(count, per * group, size).astype(BF16)
        if k == 0:
            row_recv[h][0] = row_send[h, 0]
        exchange(row_send.at[h], row_recv[h], row_ssem.at[h], row_rsem.at[h], -1, peers)

    for k, (first, count, peers) in enumerate(groups):
        arrived(idx_recv.at[pl.ds(first + (k == 0), len(peers))], idx_rsem.at[k])
        span_k = slice(first * group, (first + count) * group)
        target = idx_recv[first, :, span_k]
        for e in range(first + 1, first + count):
            target = target + idx_recv[e, :, span_k]
        mat = jnp.where(row_ids[:, : count * group] == target, 1.0, 0.0).astype(BF16)
        place_mat[:, span_k] = mat
        answer(k, 0)
    for h in range(1, halves):
        for k in (1, 0):
            answer(k, h)

    rows_all = per * group
    n_vis = vt * size
    vis_load.wait()
    row_id = lax.broadcasted_iota(jnp.int32, (rows_all, n_vis), 0)
    vis_id = lax.broadcasted_iota(jnp.int32, (rows_all, n_vis), 1)
    live = (vis_id < count_s[0, 0]) & (row_id % vt == vis_id // size)
    first_slot = (row_id // vt) % nnz == 0
    first_out = (lax.broadcasted_iota(jnp.int32, (rows_all, 2 * size), 0) // vt) % nnz == 0
    for h in range(halves):
        con_buf[h, fpb] = jnp.zeros((rows_all, size), BF16)
    arrived(wv, local_sem.at[local_sem.shape[0] - 1])

    for h in range(halves):
        arrived(row_recv[h].at[pl.ds(1, nfx - 1)], row_rsem.at[h])
        measured = []
        for p in range(2):
            for c in range(per):
                both = vis_v[h * per + c].astype(F32)
                measured.append(jnp.broadcast_to(both[p : p + 1], (slots, n_vis)))
        measured = jnp.concatenate(measured, axis=0)
        sums = [None, None]
        for q in range(fpb // 2):
            x = jnp.concatenate(
                [row_recv[h][slot_s[2 * q]], row_recv[h][slot_s[2 * q + 1]]], axis=1
            )
            for n in range(nnz):
                term = dot_nt(x, wv[q, n].reshape(n_vis, 2 * size))
                sums[n] = term if sums[n] is None else sums[n] + term
        mixed = jnp.where(first_slot, sums[0], sums[1])
        later = pltpu.roll(mixed, rows_all - vt, 0)
        earlier = pltpu.roll(mixed, vt, 0)
        predicted = mixed + jnp.where(first_slot, later, earlier)
        residual = jnp.where(live, predicted - measured, 0.0).astype(BF16)
        for q in range(fpb // 2):
            terms = [dot(residual, wv[q, n].reshape(n_vis, 2 * size)) for n in range(nnz)]
            out = jnp.where(first_out, terms[0], terms[1]).astype(BF16)
            con_buf[h, 2 * q] = out[:, :size]
            con_buf[h, 2 * q + 1] = out[:, size:]
        for k in range(nfx):
            con_send[h, k] = con_buf[h, inv_s[k]]
        con_recv[h, 0] = con_send[h, 0]
        exchange(con_send.at[h], con_recv.at[h], con_ssem.at[h], con_rsem.at[h])

    def flipped(table):
        return jnp.concatenate(
            [
                jnp.concatenate([table[:size, :size], table[size:, :size]], axis=1),
                jnp.concatenate([table[:size, size:], table[size:, size:]], axis=1),
            ],
            axis=0,
        )

    right_back = (flipped(tab[0]), flipped(tab[1]))
    left_back = tuple(dot(tab[k, :size, :], place_mat[...]).astype(BF16) for k in range(2))
    lane_id = lax.broadcasted_iota(jnp.int32, (1, size), 1)
    quarter = size // 4
    block = 2 * (quarter + 32) + 2 * per * 16
    for h in range(halves):
        arrived(con_recv.at[h, pl.ds(1, nfx - 1)], con_rsem.at[h])
        own_rows = per * slots
        incoming = jnp.concatenate(
            [
                con_recv[h, :, p * own_rows : (p + 1) * own_rows, :].reshape(nfx * own_rows, size)
                for p in range(2)
            ],
            axis=1,
        )
        half = dot(incoming, right_back[0]) + dot(incoming, right_back[1])
        half = half.reshape(nfx, per, slots, 2 * size)
        half = jnp.concatenate(
            [
                jnp.concatenate(
                    [half[:, c : c + 1, :, p * size : (p + 1) * size] for p in range(2)], axis=1
                ).reshape(nfx * group, size)
                for c in range(per)
            ],
            axis=1,
        )
        grad = dot3(left_back, split(half))
        edges = [jnp.zeros((quarter, size), F32) for _ in range(2)]
        for c in range(per):
            stepped = sky_v[h * per + c].astype(F32) - STEP * grad[:, c * size : (c + 1) * size]
            shr[h * per + c] = stepped
            high = stepped.astype(BF16)
            st_bf[h, c] = high
            hi_buf[h, c, 16 : 16 + size, :size] = high
            for fold in range(4):
                at = 32 * fold + 16 * c
                part = stepped[fold * quarter : (fold + 1) * quarter]
                hit = (lane_id >= at) & (lane_id < at + 16)
                for e, turn in enumerate((at, (at + 16) % size)):
                    moved = pltpu.roll(part, turn, 1) if turn else part
                    edges[e] = jnp.where(hit, moved, edges[e])
        for e in range(2):
            edge_send[h, e] = edges[e].astype(BF16)

        first, last = pl.ds(0, 16), pl.ds(quarter - 16, 16)
        def send(src, at, count, device):
            pltpu.make_async_remote_copy(
                src_ref=src,
                dst_ref=halo_recv.at[h, pl.ds(at, count)],
                send_sem=halo_ssem.at[h],
                recv_sem=halo_rsem.at[h],
                device_id=device,
                device_id_type=MESH,
            ).start()

        for c in range(per):
            send(st_bf.at[h, c], c * size, size, mate)
        for who, where in ((0, blk), (1, 1 - blk)):
            fr = per * size + who * block
            fl, top = fr + quarter + 32, fr + 2 * (quarter + 32)
            bottom = top + per * 16
            send(edge_send.at[h, 0, first], fr + 16 + quarter, 16, (up, left, where))
            send(edge_send.at[h, 1, first], fl + 16 + quarter, 16, (up, right, where))
            send(edge_send.at[h, 0, last], fr, 16, (down, left, where))
            send(edge_send.at[h, 1, last], fl, 16, (down, right, where))
            send(edge_send.at[h, 0], fr + 16, quarter, (fy, left, where))
            send(edge_send.at[h, 1], fl + 16, quarter, (fy, right, where))
            for c in range(per):
                send(st_bf.at[h, c, pl.ds(0, 16)], bottom + 16 * c, 16, (up, fx, where))
                send(st_bf.at[h, c, pl.ds(size - 16, 16)], top + 16 * c, 16, (down, fx, where))

    tall = size + 32
    streams = 2 * per
    in_top, in_bottom = fy > 0, fy < nfy - 1
    row_tall = lax.broadcasted_iota(jnp.int32, (tall, 1), 0)
    rows_live = ((row_tall >= 16) | in_top) & ((row_tall < 16 + size) | in_bottom)
    zeros8 = jnp.zeros((8, size), F32)
    levels = thr_v.shape[0]
    thr_copy.wait_recv()
    for who, part in enumerate((thr_v, thr_mate)):
        for c in range(n_chan):
            for level in range(levels):
                at = (who * n_chan + c) * levels + level
                value = part[level : level + 1, c : c + 1]
                bounds[at : at + 1, :] = jnp.broadcast_to(value, (1, size))
    for buf in (ybuf, zbuf):
        for q in range(streams):
            for level in range(1, levels):
                buf[q, level, 0:8, :] = zeros8
                buf[q, level, 8 + tall : 16 + tall, :] = zeros8
    smooth_load.wait()
    thr_copy.wait_send()
    arrived(idx_send.at[pl.ds(1, nfx - 1)], idx_ssem.at[0])
    for h in range(halves):
        arrived(row_send.at[h, pl.ds(1, nfx - 1)], row_ssem.at[h])
        arrived(con_send.at[h, pl.ds(1, nfx - 1)], con_ssem.at[h])
    pieces = [(0, 0, 16, 3), (16 + size, 16 + quarter, 16, 0)]
    pieces += [(16 + k * quarter, 16, quarter, k) for k in range(4)]

    def summed(ref, at, count, s):
        x = ref[at : at + count, :]
        return (ref[at - s : at - s + count, :] + x) + (ref[at + s : at + s + count, :] + x)

    for h in range(halves):
        arrived(halo_recv.at[h], halo_rsem.at[h])
        for who in range(2):
            fr = per * size + who * block
            fl, top = fr + quarter + 32, fr + 2 * (quarter + 32)
            bottom = top + per * 16
            from_left = halo_recv[h, fl : fl + quarter + 32].astype(F32)
            from_right = halo_recv[h, fr : fr + quarter + 32].astype(F32)
            for c in range(per):
                q = who * per + c
                if who == 1:
                    hi_buf[h, q, 16 : 16 + size, :size] = halo_recv[h, c * size : (c + 1) * size]
                hi_buf[h, q, 0:16, :size] = jnp.where(
                    in_top, halo_recv[h, top + 16 * c : top + 16 * c + 16].astype(F32), 0.0
                ).astype(BF16)
                hi_buf[h, q, 16 + size :, :size] = jnp.where(
                    in_bottom, halo_recv[h, bottom + 16 * c : bottom + 16 * c + 16].astype(F32), 0.0
                ).astype(BF16)
                for to, start, count, fold in pieces:
                    at = 32 * fold + 16 * c
                    r = from_right[start : start + count]
                    r = pltpu.roll(r, size - at, 1) if at else r
                    l = pltpu.roll(from_left[start : start + count], (2 * size - 16 - at) % size, 1)
                    side = jnp.where(lane_id < 64, r, l)
                    if to in (0, 16 + size):
                        side = jnp.where(rows_live[to : to + count], side, 0.0)
                    hi_buf[h, q, to : to + count, size:] = side.astype(BF16)
        for t in range(levels // 2):
            span = slice(2 * t * size, 2 * (t + 1) * size)
            result = dot(hi_buf[h].reshape(streams * tall, 2 * size), smooth[:, span])
            for q in range(streams):
                for e in range(2):
                    ybuf[q, 2 * t + e, 8 : 8 + tall, :] = result[
                        q * tall : (q + 1) * tall, e * size : (e + 1) * size
                    ]
        for q in range(streams):
            who, c = q // per, h * per + q % per
            sources = [ybuf.at[q, 0]]
            for level in range(1, levels):
                source, dest = ybuf.at[q, level], zbuf.at[q, level]
                reach = 2 ** (level + 1) - 2
                for step in range(level):
                    s = 2**step
                    reach -= s if step else 0
                    low, top = (24 - reach) // 8 * 8, (24 + size + reach + 7) // 8 * 8
                    for at, stop in ((low, 24), (24 + size, top)):
                        part = summed(source, at, stop - at, s)
                        dest[at:stop, :] = jnp.where(rows_live[at - 8 : stop - 8], part, 0.0)
                    for at in range(24, 24 + size, 32):
                        dest[at : at + 32, :] = summed(source, at, 32, s)
                    source, dest = dest, source
                sources.append(source)
            for at in range(0, size, 16):
                rows = slice(at, at + 16)
                base = (q % per) * size + at
                value = shr[c, rows, :] if who == 0 else halo_recv[h, base : base + 16].astype(F32)
                coarse = value
                for level in range(levels):
                    at_bound = (who * n_chan + c) * levels + level
                    bound = bounds[at_bound : at_bound + 1, :]
                    finer = summed(sources[level], 24 + at, 16, 2**level)
                    value = value - jnp.minimum(jnp.maximum(coarse - finer, -bound), bound)
                    coarse = finer
                if who == 0:
                    shr[c, rows, :] = value
                else:
                    other[c, rows, :] = value

    for h in range(halves):
        arrived(halo_recv.at[h], halo_ssem.at[h])


def last_kernel(shr, other, mu_s, out_ref, gpart, gtot, xs):
    n_chan, size, _ = shr.shape
    total = 2 * n_chan
    chunk = 16
    pairs = [(a, b) for a in range(total) for b in range(a, total)]

    def step(i, sums):
        rows = pl.ds(pl.multiple_of(i * chunk, chunk), chunk)
        vals = [shr[c, rows, :] for c in range(n_chan)]
        vals += [other[c, rows, :].astype(F32) for c in range(n_chan)]
        news = []
        for k, (a, b) in enumerate(pairs):
            prod = vals[a] * vals[b]
            news.append(sums[k] + (prod[:8] + prod[8:]))
        return tuple(news)

    sums = lax.fori_loop(
        0, size // chunk, step, tuple(jnp.zeros((8, size), F32) for _ in pairs)
    )
    for (a, b), value in zip(pairs, sums):
        value = jnp.sum(value, axis=0, keepdims=True)
        gpart[a * total + b : a * total + b + 1, :] = value
        if a != b:
            gpart[b * total + a : b * total + a + 1, :] = value
    gtot[...] = jnp.broadcast_to(jnp.sum(gpart[...], axis=1, keepdims=True), gtot.shape)

    mu = mu_s[0] * float(size * size)
    mat = {}
    for a, b in pairs:
        value = jnp.broadcast_to(gtot[a * total + b : a * total + b + 1, :], (total, size))
        mat[a, b] = value + mu if a == b else value
    rhs = [gtot[c * total : (c + 1) * total, :] for c in range(total)]
    inverse = [None] * total
    for k in range(total):
        inverse[k] = 1.0 / mat[k, k]
        for i in range(k + 1, total):
            factor = mat[k, i] * inverse[k]
            for j in range(i, total):
                mat[i, j] = mat[i, j] - factor * mat[k, j]
            rhs[i] = rhs[i] - factor * rhs[k]
    solved = [None] * total
    for k in range(total - 1, -1, -1):
        value = rhs[k]
        for i in range(k + 1, total):
            value = value - mat[k, i] * solved[i]
        solved[k] = value * inverse[k]
        xs[k * total : (k + 1) * total, :] = solved[k]

    coeffs = [
        [jnp.broadcast_to(xs[c * total + d : c * total + d + 1, :], (8, size)) for c in range(total)]
        for d in range(n_chan)
    ]

    def finish(i, carry):
        rows = pl.ds(pl.multiple_of(i * chunk, chunk), chunk)
        vals = [shr[c, rows, :] for c in range(n_chan)]
        vals += [other[c, rows, :].astype(F32) for c in range(n_chan)]
        for d in range(n_chan):
            for h in range(2):
                value = coeffs[d][0] * vals[0][h * 8 : h * 8 + 8]
                for c in range(1, total):
                    value = value + coeffs[d][c] * vals[c][h * 8 : h * 8 + 8]
                out_ref[d, pl.ds(pl.multiple_of(i * chunk + h * 8, 8), 8), :] = value
        return carry

    lax.fori_loop(0, size // chunk, finish, 0)


def body(sizes, sky, vis, weights, tiles, lists, count, threshold, weight):
    nfx, nfy, nblk, fpb, vt, nnz, halves = sizes
    n_chan, size, _ = sky.shape
    per = n_chan // halves
    rows = per * 2 * vt * nnz
    lanes = nfx * 2 * vt * nnz
    hbm = pl.BlockSpec(memory_space=pltpu.HBM)
    smem = pl.BlockSpec(memory_space=pltpu.SMEM)
    vmem = pl.BlockSpec(memory_space=pltpu.VMEM)
    tall = size + 48
    levels = threshold.shape[0]
    sem = pltpu.SemaphoreType.DMA
    shr, other = pl.pallas_call(
        functools.partial(kernel, sizes),
        out_shape=[
            jax.ShapeDtypeStruct((n_chan, size, size), F32),
            jax.ShapeDtypeStruct((n_chan, size, size), F32),
        ],
        in_specs=[hbm] * 5 + [smem, hbm, hbm, hbm],
        out_specs=[vmem, vmem],
        scratch_shapes=[
            pltpu.SMEM((vt, nnz, fpb), jnp.int32),
            pltpu.SMEM((fpb,), jnp.int32),
            pltpu.VMEM((n_chan, size, size), BF16),
            pltpu.VMEM((n_chan, 2, vt * size), BF16),
            pltpu.VMEM((fpb // 2, nnz, vt, size, 2 * size), BF16),
            pltpu.VMEM((2, 2 * size, 2 * size), BF16),
            pltpu.VMEM((2 * size, levels * size), BF16),
            pltpu.VMEM((nfx, 1, lanes), jnp.int32),
            pltpu.VMEM((nfx, 1, lanes), jnp.int32),
            pltpu.VMEM((2 * size, n_chan * size), BF16),
            pltpu.VMEM((halves, nfx, rows, size), BF16),
            pltpu.VMEM((nfx, rows, size), BF16),
            pltpu.VMEM((nfx, rows, size), BF16),
            pltpu.VMEM((halves, fpb + 1, rows, size), BF16),
            pltpu.VMEM((halves, nfx, rows, size), BF16),
            pltpu.VMEM((halves, nfx, rows, size), BF16),
            pltpu.SMEM((nfx,), jnp.int32),
            pltpu.SMEM((fpb,), jnp.int32),
            pltpu.VMEM((2 * size, lanes), BF16),
            pltpu.VMEM((halves, per, size, size), BF16),
            pltpu.VMEM((halves, 2, size // 4, size), BF16),
            pltpu.VMEM((halves, per * size + 4 * (size // 4 + 32 + per * 16), size), BF16),
            pltpu.VMEM((halves, 2 * per, size + 32, 2 * size), BF16),
            pltpu.VMEM((2 * per, levels, tall, size), F32),
            pltpu.VMEM((2 * per, levels, tall, size), F32),
            pltpu.VMEM(threshold.shape, F32),
            pltpu.VMEM(threshold.shape, F32),
            pltpu.VMEM((2 * n_chan * levels, size), F32),
            sem((9,)),
            sem((1,)),
            sem((2,)),
            sem((halves,)),
            sem((halves,)),
            sem((halves,)),
            sem((halves,)),
            sem((halves,)),
            sem((halves,)),
            sem((2,)),
        ],
        compiler_params=pltpu.CompilerParams(
            collective_id=0, has_side_effects=True, vmem_limit_bytes=24 * 2**20
        ),
    )(
        pinned(sky),
        pinned(vis[0, 0]),
        pinned(weights[0, 0]),
        pinned(tiles[0, 0].transpose(1, 2, 0)),
        pinned(lists.reshape(-1)),
        count,
        pinned(threshold),
        pinned(jnp.asarray(tables(size))),
        pinned(jnp.asarray(smoothers(size, levels, 16))),
    )
    square = pltpu.VMEM((4 * n_chan * n_chan, size), F32)
    return pl.pallas_call(
        last_kernel,
        out_shape=jax.ShapeDtypeStruct((n_chan, size, size), F32),
        in_specs=[vmem, vmem, smem],
        out_specs=vmem,
        scratch_shapes=[square, square, square],
        compiler_params=pltpu.CompilerParams(vmem_limit_bytes=8 * 2**20),
    )(shr, other, weight.reshape(1))


def solution(mesh):
    in_specs = (
        P("blk", "fy", "fx"),
        P("fy", "fx", "blk", None, None),
        P("fy", "fx", None, None, None, None, None),
        P("fy", "fx", None, None, None),
        P("fy", "fx", None),
        P("fy", "fx"),
        P(None, "blk"),
        P(),
    )

    def step(*args):
        fpb, vt, nnz = args[3].shape[2:]
        sizes = (mesh.shape["fx"], mesh.shape["fy"], mesh.shape["blk"], fpb, vt, nnz, 2)
        return body(sizes, *args)

    return jax.shard_map(
        step, mesh=mesh, in_specs=in_specs, out_specs=P("blk", "fy", "fx"), check_vma=False
    )
```
